256 devices in a mesh: seq: 32 (over y_lo, z, core), batch: 8 (over x, y_hi).
Axes of the slice: x: 4, y: 4 (y_hi: 2, y_lo: 2; y = y_hi * 2 + y_lo), z: 8, core: 2. Of those that a mesh axis runs over, the one named last changes fastest.
Arguments:
- embedded: bfloat16 [32768, 1024], P(('batch', 'seq')), parts along dimension 0, may hold values from -6 to 6
- w_qkv: bfloat16 [2, 1024, 3072], P(None, 'seq'), may hold values from -0.1875 to 0.1875
- w_out: bfloat16 [2, 1024, 1024], P(None, 'seq'), may hold values from -0.1875 to 0.1875
- w_pos: bfloat16 [2, 1024, 1024], P(None, None, 'seq'), may hold values from -0.1875 to 0.1875
- bias_content: float32 [2, 1024], replicated, may hold values from -3 to 3
- bias_position: float32 [2, 1024], replicated, may hold values from -3 to 3
- norm_gain: float32 [2, 1024], replicated, may hold values from 0.5 to 1.5
- norm_offset: float32 [2, 1024], replicated, may hold values from -2 to 2
- table: bfloat16 [12288, 1024], P('seq'), may hold values from -1 to 1
- targets: int32 [32768], P('batch'), parts along dimension 0, may hold values from 0 to 12287
- valid_length: int32 [8], P('batch'), parts along dimension 0, may hold values from 3969 to 4096
Outputs:
- hidden_out: bfloat16 [32768, 1024], P(('batch', 'seq')), parts along dimension 0
- token_loss: float32 [32768], P(('batch', 'seq')), parts along dimension 0
- loss_value: float32 [8], P('batch'), parts along dimension 0
The draws below stay inside these ranges and needn't reach their ends.
There are 8 independent parts, one for each index of `batch`. The reference program is written for one: setup_inputs(seed, part) draws one part's arguments, and reference() takes and returns one part's arrays. A program takes and returns all parts, laid end to end along the dimension named above; an argument that names none is the same for every part. Nothing has to cross between parts.
All inputs are finite; a program needn't handle non-finite values.
Results may differ from the reference program's by a relative error of at most 0.006.
Values may be sent and summed in bfloat16 or wider, within the bound.
A program may use at most 64 MiB of HBM per device.

```python
import math
import jax
import jax.numpy as jnp
import numpy as np
from jax import lax

D = 1024
HEADS = 16
HEAD = 64
LAYERS = 2
TOK_DEV = 128
TOKENS = 4096
VOCAB = 12288
N_SEQ = 32


def draw_table(key, part):
    col_key = jax.random.fold_in(jax.random.fold_in(key, 7), 1)
    base_key = jax.random.fold_in(jax.random.fold_in(key, 7), 2)
    col_scale = jnp.exp(jax.random.uniform(col_key, (D,), minval=-0.6, maxval=0.6))
    base_draw = jnp.clip(jax.random.normal(base_key, (VOCAB, D)), -6.0, 6.0)
    values = 3.0 * base_draw * col_scale[None, :] / math.sqrt(D)
    values = jnp.clip(values, -1.0, 1.0)
    return values.astype(jnp.bfloat16)


def with_ends(entries, key, least, high):
    place = [jax.random.randint(jax.random.fold_in(key, axis), (), 0, length) for axis, length in enumerate(entries.shape)]
    main_axis = entries.shape.index(max(entries.shape))
    beside = place[:main_axis] + [(place[main_axis] + 1) % entries.shape[main_axis]] + place[main_axis + 1:]
    return entries.at[tuple(place)].set(least).at[tuple(beside)].set(high)


def levels(key, shape, cuts, least, largest):
    loudness = 1.0
    for dim, blocks in cuts:
        heights = jax.random.uniform(jax.random.fold_in(jax.random.fold_in(key, 6), dim), (blocks,), jnp.float32, least / len(cuts), largest / len(cuts))
        loudness = loudness * jnp.repeat(jnp.exp(heights), shape[dim] // blocks).reshape((-1,) + (1,) * (len(shape) - 1 - dim))
    return loudness


def rank_bounds(number_of, lean):
    loads = [(1 << 20) // math.isqrt(grade ** lean) + 1 for grade in range(1, number_of + 1)]
    deviation = 1 + sum(loads) // (1 << 30)
    return np.cumsum(np.array([max(1, weight // deviation) for weight in loads]))


def ranked(rng, dims, count, slope):
    listing = rank_bounds(count, slope)
    lot = jax.random.randint(jax.random.fold_in(rng, 1), dims, 0, int(listing[count - 1]))
    grade = jnp.searchsorted(jnp.asarray(listing, jnp.int32), lot, side="right")
    return jax.random.permutation(jax.random.fold_in(rng, 2), count)[grade].astype(jnp.int32)


def bell_draw(rng, dims, width, reach, cuts=(), dtype=jnp.bfloat16):
    level = levels(rng, dims, cuts, -0.22, 0.18) if cuts else 1.0
    result = jax.random.normal(rng, dims, jnp.float32) * width * level
    return jnp.minimum(jnp.maximum(result, -reach), reach).astype(dtype)


def setup_inputs(seed: int = 0, part: int = 0) -> dict:
    key_of = jax.random.split(jax.random.key(seed), 12)
    part_splits = jax.random.split(jax.random.fold_in(key_of[11], part), 12)
    return {
        "embedded": bell_draw(part_splits[0], (TOKENS, D), 1.0, 6.0, ((0, 32),)),
        "w_qkv": bell_draw(key_of[1], (LAYERS, D, 3 * D), D ** -0.5, 0.1875, ((1, 32),)),
        "w_out": bell_draw(key_of[2], (LAYERS, D, D), D ** -0.5, 0.1875, ((1, 32),)),
        "w_pos": bell_draw(key_of[3], (LAYERS, D, D), D ** -0.5, 0.1875, ((2, 32),)),
        "bias_content": bell_draw(key_of[4], (LAYERS, D), 0.5, 3.0, (), jnp.float32),
        "bias_position": bell_draw(key_of[5], (LAYERS, D), 0.5, 3.0, (), jnp.float32),
        "norm_gain": jnp.clip(1.0 + 0.1 * jax.random.normal(key_of[6], (LAYERS, D), jnp.float32), 0.5, 1.5),
        "norm_offset": bell_draw(key_of[7], (LAYERS, D), 0.3, 2.0, (), jnp.float32),
        "table": draw_table(jax.random.fold_in(key_of[11], 71), part),
        "targets": with_ends(ranked(part_splits[9], (TOKENS,), VOCAB, 2), jax.random.fold_in(part_splits[9], 3), 0, VOCAB - 1).astype(jnp.int32),
        "valid_length": jax.random.randint(part_splits[10], (1,), TOKENS - TOK_DEV + 1, TOKENS + 1).astype(jnp.int32),
    }


norm_eps = 1e-05

def sinusoid(row_count, model_width):
    distance = jnp.arange(row_count - 1, -1, -1).astype(jnp.float32)
    inverse = 1.0 / 10000.0 ** (jnp.arange(0, model_width, 2).astype(jnp.float32) / model_width)
    angles = distance[:, None] * inverse[None, :]
    return jnp.concatenate([jnp.sin(angles), jnp.cos(angles)], axis=1).astype(jnp.bfloat16)

def rel_shift(scores):
    leading = scores.shape[:-2]
    row_count, col_count = (scores.shape[-2], scores.shape[-1])
    padded = jnp.pad(scores, [(0, 0)] * len(leading) + [(0, 0), (1, 0)])
    flattened = padded.reshape(leading + (row_count * (col_count + 1),))[..., row_count:]
    return flattened.reshape(leading + (row_count, col_count))

def layer_norm(values, gain_row, offset_row):
    row_mean = lax.optimization_barrier(jnp.mean(values, -1, keepdims=True))
    centred = values - row_mean
    spread = lax.optimization_barrier(jnp.mean(centred * centred, -1, keepdims=True))
    return centred * lax.rsqrt(spread + norm_eps) * gain_row + offset_row

def reference(embedded, w_qkv, w_out, w_pos, bias_content, bias_position, norm_gain, norm_offset, table, targets, valid_length):
    blocks = N_SEQ
    block_len = TOK_DEV
    pos_table = sinusoid(2 * block_len, D)
    query_idx = jnp.arange(block_len)[:, None]
    key_idx = jnp.arange(2 * block_len)[None, :]
    has_memory = jnp.arange(blocks)[:, None, None] > 0
    allowed = (key_idx <= query_idx + block_len)[None] & ((key_idx >= block_len)[None] | has_memory)
    hidden = embedded
    shape_heads = (blocks, block_len, HEADS, HEAD)
    empty_block = jnp.zeros((1, block_len, HEADS, HEAD), jnp.bfloat16)
    for layer_idx in range(LAYERS):
        mixed_rows = jnp.dot(hidden, w_qkv[layer_idx], preferred_element_type=jnp.float32)
        query_rows = mixed_rows[:, :D]
        q_content = (query_rows + bias_content[layer_idx]).astype(jnp.bfloat16).reshape(shape_heads)
        q_position = (query_rows + bias_position[layer_idx]).astype(jnp.bfloat16).reshape(shape_heads)
        key_rows = mixed_rows[:, D:2 * D].astype(jnp.bfloat16).reshape(shape_heads)
        value_rows = mixed_rows[:, 2 * D:].astype(jnp.bfloat16).reshape(shape_heads)
        keys_all = jnp.concatenate([jnp.concatenate([empty_block, key_rows[:-1]], 0), key_rows], 1)
        values_all = jnp.concatenate([jnp.concatenate([empty_block, value_rows[:-1]], 0), value_rows], 1)
        pos_keys = jnp.dot(pos_table, w_pos[layer_idx], preferred_element_type=jnp.float32).astype(jnp.bfloat16)
        pos_keys = pos_keys.reshape(2 * block_len, HEADS, HEAD)
        content = jnp.einsum('nqhd,nkhd->nhqk', q_content.astype(jnp.float32), keys_all.astype(jnp.float32))
        position = rel_shift(jnp.einsum('nqhd,khd->nhqk', q_position.astype(jnp.float32), pos_keys.astype(jnp.float32)))
        scores = (content + position) * HEAD ** (-0.5)
        exp_scores = jnp.where(allowed[:, None], jnp.exp(scores), 0.0)
        attn_probs = (exp_scores / lax.optimization_barrier(jnp.sum(exp_scores, -1, keepdims=True))).astype(jnp.bfloat16)
        attended = jnp.einsum('nhqk,nkhd->nqhd', attn_probs.astype(jnp.float32), values_all.astype(jnp.float32))
        attended = attended.astype(jnp.bfloat16).reshape(TOKENS, D)
        projected = jnp.dot(attended, w_out[layer_idx], preferred_element_type=jnp.float32)
        hidden = layer_norm(hidden.astype(jnp.float32) + projected, norm_gain[layer_idx], norm_offset[layer_idx]).astype(jnp.bfloat16)

    def block_loss(operands):
        rows_block, wanted = operands
        logits = jnp.dot(rows_block, table.T, preferred_element_type=jnp.float32)
        exp_sums = lax.optimization_barrier(jnp.sum(jnp.exp(logits), 1))
        picked = jnp.take_along_axis(logits, wanted[:, None].astype(jnp.int32), 1)[:, 0]
        return jnp.log(exp_sums) - picked
    per_token = lax.map(block_loss, (hidden.reshape(blocks, block_len, D), targets.reshape(blocks, block_len))).reshape(TOKENS)
    is_live = jnp.arange(TOKENS) < valid_length[0]
    token_loss = jnp.where(is_live, per_token, 0.0)
    loss_value = (jnp.sum(token_loss) / valid_length[0].astype(jnp.float32)).reshape(1)
    hidden_out = jnp.where(is_live[:, None], hidden, jnp.zeros_like(hidden))
    return (hidden_out, token_loss, loss_value)
```

```python
import functools

import jax
import jax.numpy as jnp
import numpy as np
from jax import lax
from jax.experimental import pallas as pl
from jax.experimental.pallas import tpu as pltpu
from jax.sharding import PartitionSpec as P

HEADS = 16
LAYERS = 2
D = 1024
BLK = 128
NZ = 8
SHARD = 32
WORDS = 384
PO = 256 + D
EPS = 1e-05
MESH = pl.DeviceIdType.MESH
BF = jnp.bfloat16
F32 = jnp.float32


def pos_table_t(row_count, model_width):
    distance = np.arange(row_count - 1, -1, -1).astype(np.float32)
    inverse = np.float32(1.0) / np.float32(10000.0) ** (
        np.arange(0, model_width, 2).astype(np.float32) / np.float32(model_width)
    )
    angles = distance[:, None] * inverse[None, :].astype(np.float32)
    table = np.concatenate([np.sin(angles), np.cos(angles)], axis=1)
    return jnp.asarray(table.T, F32).astype(BF)


def kernel(
    emb, wqkv, po_in, bias_c, bias_p, gain, offset, table, targets, vlen,
    hid_out, tl_out, loss_out,
    W, POW, T, X0, X1, QC, QP, K, V, ATT, Y, HALL, STL, ST, PART,
    lsem, ring_r, y_r, d_r, w_s, halo_s, halo_r, t_s, t_r, h_s, h_r, st_s, st_r, p_s, p_r,
):
    i = lax.axis_index("seq")
    b = lax.axis_index("batch")
    c = i % 2
    z = (i // 2) % NZ
    y = i // (2 * NZ)
    sgn = 1 - 2 * c

    def dev(yy, zz, cc):
        return (yy * NZ + zz) * 2 + cc

    def zoff(k):
        return (z + 2 * NZ + k) % NZ

    fwd = {"seq": dev(y, zoff(sgn), c)}
    bwd = {"seq": dev(y, zoff(-sgn), c)}
    partner = {"seq": dev(y, z, 1 - c)}
    diag = {"seq": dev(1 - y, z, 1 - c)}
    near = {"seq": dev(1 - y, z, c)}
    far = {"seq": dev(1 - y, z, c), "batch": (b // 2) * 2 + 1 - b % 2}
    nxt = {"seq": (i + 1) % 32}
    prv = {"seq": (i + 31) % 32}

    def rcopy(src, dst, ss, rs, to):
        return pltpu.make_async_remote_copy(
            src_ref=src, dst_ref=dst, send_sem=ss, recv_sem=rs, device_id=to, device_id_type=MESH
        )

    loc = [
        pltpu.make_async_copy(wqkv.at[0], W.at[0, y, z, c], lsem.at[0]),
        pltpu.make_async_copy(emb, X0.at[1], lsem.at[1]),
        pltpu.make_async_copy(po_in, POW.at[:, y, z, c], lsem.at[2]),
        pltpu.make_async_copy(wqkv.at[1], W.at[1, y, z, c], lsem.at[3]),
        pltpu.make_async_copy(table, T.at[y, c], lsem.at[4]),
    ]
    for cp in loc:
        cp.start()

    barrier = pltpu.get_barrier_semaphore()
    for k in range(1, NZ):
        pl.semaphore_signal(barrier, inc=1, device_id={"seq": dev(y, zoff(k), c)}, device_id_type=MESH)
    for peer in (partner, diag, near, far, nxt, prv):
        pl.semaphore_signal(barrier, inc=1, device_id=peer, device_id_type=MESH)
    pl.semaphore_wait(barrier, NZ - 1 + 6)

    def stream(si, yy, zz):
        if si in (3, 7):
            return POW.at[si // 4, yy, zz, c]
        layer, col = (0, si) if si < 3 else (1, si - 4)
        return W.at[layer, yy, zz, c, :, pl.ds(col * D, D)]

    def own(group):
        for si in group:
            s = stream(si, y, z)
            rcopy(s, s, w_s.at[si, 0], ring_r.at[si, 0], fwd).start()
            rcopy(s, s, w_s.at[si, 1], ring_r.at[si, 4], bwd).start()
            rcopy(s, s, w_s.at[si, 2], y_r.at[si, 0], near).start()

    def step(group, d):
        for si in group:
            s = stream(si, y, zoff(-sgn * d))
            rcopy(s, s, w_s.at[si, 0], ring_r.at[si, d - 1], fwd).wait_recv()
            if d < 4:
                rcopy(s, s, w_s.at[si, 0], ring_r.at[si, d], fwd).start()
            rcopy(s, s, w_s.at[si, 3], y_r.at[si, 1], far).start()
            if d < 4:
                s = stream(si, y, zoff(sgn * d))
                rcopy(s, s, w_s.at[si, 1], ring_r.at[si, 3 + d], bwd).wait_recv()
                if d < 3:
                    rcopy(s, s, w_s.at[si, 1], ring_r.at[si, 4 + d], bwd).start()
                rcopy(s, s, w_s.at[si, 2], y_r.at[si, 0], near).start()

    def d2d_own(group):
        for si in group:
            s = stream(si, y, pl.ds(0, NZ))
            rcopy(s, s, w_s.at[si, 4], d_r.at[si, 0], partner).start()

    def d2d_other(group):
        for si in group:
            s4 = stream(si, 1 - y, pl.ds(0, 4))
            rcopy(s4, s4, w_s.at[si, 2], y_r.at[si, 0], near).wait_recv()
            rcopy(s4, s4, w_s.at[si, 3], y_r.at[si, 1], far).wait_recv()
            s = stream(si, 1 - y, pl.ds(0, NZ))
            rcopy(s, s, w_s.at[si, 5], d_r.at[si, 1], partner).start()

    def finish(group):
        for si in group:
            s = stream(si, y, pl.ds(0, NZ))
            rcopy(s, s, w_s.at[si, 4], d_r.at[si, 0], partner).wait_recv()
            rcopy(s, s, w_s.at[si, 5], d_r.at[si, 1], partner).wait_recv()

    def drain(group):
        for si in group:
            for k, n in ((0, 4), (1, 3), (2, 4), (3, 4), (4, 8), (5, 8)):
                s = stream(si, y, pl.ds(0, n))
                rcopy(s, s, w_s.at[si, k], ring_r.at[si, 0], fwd).wait_send()

    low = lax.broadcasted_iota(jnp.int32, (BLK, BLK), 1) < 64
    rows = lax.broadcasted_iota(jnp.int32, (BLK, 2 * BLK), 0)
    cols = lax.broadcasted_iota(jnp.int32, (BLK, 2 * BLK), 1)
    first_key = BLK * (1 - jnp.minimum(i, 1))
    allowed = (cols <= rows + BLK) & (cols >= first_key)

    def lanes(t, size):
        return pl.ds(pl.multiple_of(t * size, size), size)

    def weights(layer, col):
        return W[layer, :, :, :, :, pl.ds(pl.multiple_of(col, 256), 256)].reshape(D, 256)

    def queries(layer, X):
        def body(t, carry):
            sl = lanes(t, 256)
            q = jnp.dot(X[1], weights(layer, t * 256), preferred_element_type=F32)
            QC[:, sl] = (q + bias_c[layer : layer + 1, sl]).astype(BF)
            QP[:, sl] = (q + bias_p[layer : layer + 1, sl]).astype(BF)
            return carry

        lax.fori_loop(0, 4, body, 0)

    def keys_values(layer, X, part):
        row0, count = {"all": (0, 2), "own": (1, 1), "memory": (0, 1)}[part]

        def body(t, carry):
            x = X[row0 : row0 + count].reshape(count * BLK, D)
            r = pl.ds(row0 * BLK, count * BLK)
            sl = lanes(t, 256)
            K[r, sl] = jnp.dot(x, weights(layer, D + t * 256), preferred_element_type=F32).astype(BF)
            V[r, sl] = jnp.dot(x, weights(layer, 2 * D + t * 256), preferred_element_type=F32).astype(BF)
            return carry

        lax.fori_loop(0, 4, body, 0)

    def both(x):
        zero = jnp.zeros_like(x)
        return jnp.concatenate([jnp.where(low, x, zero), jnp.where(low, zero, x)], 0)

    def attend(layer, start, stop):
        def body(p, carry):
            sl = lanes(p, BLK)
            q2 = both(QC[:, sl].astype(F32)).astype(BF)
            r2 = both(QP[:, sl].astype(F32)).astype(BF)
            content = lax.dot_general(
                q2, K[:, sl], (((1,), (1,)), ((), ())), preferred_element_type=F32
            )
            pos = POW[layer, p // 4, pl.ds((p % 4) * 2, 2), :, :, 0:256].reshape(BLK, 2 * BLK)
            position = jnp.dot(r2, pos, preferred_element_type=F32)
            outs = []
            for k in range(2):
                half = slice(k * BLK, (k + 1) * BLK)
                shifted = pltpu.roll(position[half], BLK + 1, 1, stride=1, stride_axis=0)
                scores = (content[half] + shifted) * 0.125
                e = jnp.where(allowed, jnp.exp(scores), 0.0)
                outs.append((e / jnp.sum(e, -1, keepdims=True)).astype(BF))
            o = jnp.dot(jnp.concatenate(outs, 0), V[:, sl], preferred_element_type=F32)
            ATT[:, sl] = jnp.where(low, o[:BLK], o[BLK:]).astype(BF)
            return carry

        lax.fori_loop(start, stop, body, 0)

    def project(layer, X):
        def body(t, carry):
            sl = lanes(t, 256)
            w = POW[layer, :, :, :, :, pl.ds(pl.multiple_of(256 + t * 256, 256), 256)].reshape(D, 256)
            Y[:, sl] = jnp.dot(ATT[...], w, preferred_element_type=F32) + X[1, :, sl].astype(F32)
            return carry

        lax.fori_loop(0, 4, body, 0)

    def norm(layer, dst, last):
        def body(t, carry):
            r = pl.ds(pl.multiple_of(t * 32, 32), 32)
            v = Y[r, :]
            v = v - jnp.mean(v, -1, keepdims=True)
            spread = jnp.mean(v * v, -1, keepdims=True)
            h = v * lax.rsqrt(spread + EPS) * gain[layer : layer + 1, :] + offset[layer : layer + 1, :]
            dst[r, :] = h.astype(BF)
            if last:
                pos = lax.broadcasted_iota(jnp.int32, (32, D), 0) + (i * BLK + t * 32)
                hid_out[r, :] = jnp.where(pos < vlen[0], h, 0.0).astype(BF)
            return carry

        lax.fori_loop(0, 4, body, 0)

    G0, G1, G2 = (0, 1, 2), (3, 4), (5, 6, 7)

    loc[0].wait()
    own(G0)
    loc[1].wait()
    halo0 = rcopy(X0.at[1], X0.at[0], halo_s.at[0], halo_r.at[0], nxt)
    halo0.start()
    for cp in loc[2:]:
        cp.wait()
    for d in (1, 2, 3):
        step(G0, d)
    own(G1)
    step(G0, 4)
    d2d_own(G0)
    step(G1, 1)
    d2d_other(G0)
    halves = (pl.ds(0, WORDS // 2), pl.ds(WORDS // 2, WORDS // 2))
    tcopies = [
        rcopy(T.at[y, c, h], T.at[y, c, h], t_s.at[k], t_r.at[k], to)
        for k, (h, to) in enumerate(zip(halves, (near, far)))
    ] + [rcopy(T.at[y, c], T.at[y, c], t_s.at[2], t_r.at[2], partner)]
    tcopies[2].start()
    finish(G0)
    halo0.wait_recv()
    queries(0, X0)
    step(G1, 2)
    keys_values(0, X0, "all")
    step(G1, 3)
    own(G2)
    step(G1, 4)
    d2d_own(G1)
    d2d_other(G1[:1])
    finish(G1[:1])
    attend(0, 0, 3)
    step(G2, 1)
    attend(0, 3, 6)
    d2d_other(G1[1:])
    attend(0, 6, 8)
    step(G2, 2)
    project(0, X0)
    norm(0, X1.at[1], False)
    halo1 = rcopy(X1.at[1], X1.at[0], halo_s.at[1], halo_r.at[1], nxt)
    halo1.start()
    finish(G1[1:])
    queries(1, X1)
    step(G2, 3)
    step(G2, 4)
    d2d_own(G2)
    tcopies[0].start()
    tcopies[1].start()
    d2d_other(G2)
    finish(G2[:2])
    keys_values(1, X1, "own")
    halo1.wait_recv()
    keys_values(1, X1, "memory")
    finish(G2[2:])
    attend(1, 0, 8)
    tcopies[0].wait_recv()
    tcopies[1].wait_recv()
    t_other = rcopy(T.at[1 - y, c], T.at[1 - y, c], t_s.at[3], t_r.at[3], partner)
    t_other.start()
    project(1, X1)
    norm(1, HALL.at[0], True)

    hv = (pl.ds(0, BLK // 2), pl.ds(BLK // 2, BLK // 2))

    def hcopy(d, backward, half):
        src = 0 if d == 0 else (2 * d if backward else 2 * d - 1)
        dst = 2 * d + 2 if backward else 2 * d + 1
        k = (4 if backward else 0) + d
        return rcopy(
            HALL.at[src, hv[half]], HALL.at[dst, hv[half]],
            h_s.at[1 if backward else 0], h_r.at[k, half], bwd if backward else fwd,
        )

    for half in (0, 1):
        hcopy(0, False, half).start()
        hcopy(0, True, half).start()

    tcopies[2].wait_recv()
    t_other.wait_recv()

    def stats(slot, blocks):
        n = len(blocks)
        hb = HALL[slot : slot + n].reshape(n * BLK, D)
        tg = [targets[pl.ds(dev(y, zz, c), 1), :] for zz in blocks]
        tg = tg[0] if n == 1 else jnp.concatenate(tg, 1)
        word = lax.broadcasted_iota(jnp.int32, (WORDS, n * BLK), 0)

        def body(k, carry):
            sums, picks = carry
            first = dev(k // 2, z, k % 2) * WORDS
            logits = lax.dot_general(
                T[k // 2, k % 2], hb, (((1,), (1,)), ((), ())), preferred_element_type=F32
            )
            sums = sums + jnp.sum(jnp.exp(logits), 0, keepdims=True)
            picks = picks + jnp.sum(jnp.where(word == tg - first, logits, 0.0), 0, keepdims=True)
            return sums, picks

        zero = jnp.zeros((1, n * BLK), F32)
        sums, picks = lax.fori_loop(0, 4, body, (zero, zero))
        for k, zz in enumerate(blocks):
            STL[pl.ds(zz, 1), :] = sums[:, k * BLK : (k + 1) * BLK]
            STL[pl.ds(NZ + zz, 1), :] = picks[:, k * BLK : (k + 1) * BLK]

    stats(0, [z])
    for d in (1, 2, 3, 4):
        for half in (0, 1):
            hcopy(d - 1, False, half).wait_recv()
            if d < 4:
                hcopy(d, False, half).start()
                hcopy(d - 1, True, half).wait_recv()
                if d < 3:
                    hcopy(d, True, half).start()
        if d < 4:
            stats(2 * d - 1, [zoff(-sgn * d), zoff(sgn * d)])
        else:
            stats(7, [zoff(4)])

    scopies = []
    for k in range(1, NZ):
        cp = rcopy(STL, ST.at[k], st_s.at[k - 1], st_r.at[k - 1], {"seq": dev(y, zoff(k), c)})
        cp.start()
        scopies.append(cp)
    ST[0] = STL[...]
    for cp in scopies:
        cp.wait_recv()

    def add(k, total):
        return total + ST[(z + 2 * NZ - k) % NZ]

    total = lax.fori_loop(0, NZ, add, jnp.zeros((2 * NZ, BLK), F32))
    token = lax.broadcasted_iota(jnp.int32, (NZ, BLK), 0) * (2 * BLK) + (
        lax.broadcasted_iota(jnp.int32, (NZ, BLK), 1) + (y * NZ * 2 + c) * BLK
    )
    per_token = jnp.where(token < vlen[0], jnp.log(total[:NZ]) - total[NZ:], 0.0)
    mine = lax.broadcasted_iota(jnp.int32, (NZ, BLK), 0) == z
    tl_out[...] = jnp.sum(jnp.where(mine, per_token, 0.0), 0, keepdims=True)
    PART[pl.ds(2 * y + c, 1)] = per_token[None]
    pc = []
    for k, to in enumerate((partner, near, diag)):
        s = PART.at[2 * y + c]
        cp = rcopy(s, s, p_s.at[k], p_r.at[k], to)
        cp.start()
        pc.append(cp)
    for cp in pc:
        cp.wait_recv()
    loss = jnp.sum(PART[0] + PART[1] + (PART[2] + PART[3])) / vlen[0].astype(F32)
    loss_out[...] = jnp.full((1, BLK), loss, F32)

    for cp in pc + scopies:
        cp.wait_send()
    drain(G0 + G1 + G2)
    halo0.wait_send()
    halo1.wait_send()
    for cp in tcopies + [t_other]:
        cp.wait_send()
    for k, n in ((0, 4), (1, 3)):
        s = HALL.at[pl.ds(0, n)]
        rcopy(s, s, h_s.at[k], h_r.at[0, 0], fwd).wait_send()


def on_device(
    embedded, w_qkv, w_out, w_pos, bias_content, bias_position, norm_gain, norm_offset,
    table, targets, valid_length,
):
    pos_share = jnp.einsum(
        "ldc,dm->lcm", w_pos, pos_table_t(2 * BLK, D), preferred_element_type=F32
    ).astype(BF)
    po_in = jnp.concatenate([pos_share, w_out], 2)
    vmem = pl.BlockSpec(memory_space=pltpu.VMEM)
    hbm = pl.BlockSpec(memory_space=pl.ANY)
    smem = pl.BlockSpec(memory_space=pltpu.SMEM)
    DMA = pltpu.SemaphoreType.DMA
    hidden, token_loss, loss = pl.pallas_call(
        kernel,
        out_shape=(
            jax.ShapeDtypeStruct((BLK, D), BF),
            jax.ShapeDtypeStruct((1, BLK), F32),
            jax.ShapeDtypeStruct((1, BLK), F32),
        ),
        in_specs=[hbm, hbm, hbm, vmem, vmem, vmem, vmem, hbm, vmem, smem],
        out_specs=(vmem, vmem, vmem),
        scratch_shapes=[
            pltpu.VMEM((LAYERS, 2, NZ, 2, SHARD, 3 * D), BF),
            pltpu.VMEM((LAYERS, 2, NZ, 2, SHARD, PO), BF),
            pltpu.VMEM((2, 2, WORDS, D), BF),
            pltpu.VMEM((2, BLK, D), BF),
            pltpu.VMEM((2, BLK, D), BF),
            pltpu.VMEM((BLK, D), BF),
            pltpu.VMEM((BLK, D), BF),
            pltpu.VMEM((2 * BLK, D), BF),
            pltpu.VMEM((2 * BLK, D), BF),
            pltpu.VMEM((BLK, D), BF),
            pltpu.VMEM((BLK, D), F32),
            pltpu.VMEM((NZ, BLK, D), BF),
            pltpu.VMEM((2 * NZ, BLK), F32),
            pltpu.VMEM((NZ, 2 * NZ, BLK), F32),
            pltpu.VMEM((4, NZ, BLK), F32),
            DMA((5,)),
            DMA((8, 7)),
            DMA((8, 2)),
            DMA((8, 2)),
            DMA((8, 6)),
            DMA((2,)),
            DMA((2,)),
            DMA((4,)),
            DMA((4,)),
            DMA((2,)),
            DMA((7, 2)),
            DMA((NZ - 1,)),
            DMA((NZ - 1,)),
            DMA((3,)),
            DMA((3,)),
        ],
        compiler_params=pltpu.CompilerParams(
            collective_id=0, has_side_effects=True, vmem_limit_bytes=58 * 1024 * 1024
        ),
    )(
        embedded, w_qkv, po_in, bias_content, bias_position, norm_gain, norm_offset,
        table, targets.reshape(32, BLK), valid_length,
    )
    return hidden, token_loss.reshape(BLK), loss[0, :1]


def solution(mesh):
    in_specs = (
        P(("batch", "seq"), None),
        P(None, "seq", None),
        P(None, "seq", None),
        P(None, None, "seq"),
        P(),
        P(),
        P(),
        P(),
        P("seq", None),
        P("batch"),
        P("batch"),
    )
    out_specs = (P(("batch", "seq"), None), P(("batch", "seq")), P("batch"))
    return jax.shard_map(
        on_device, mesh=mesh, in_specs=in_specs, out_specs=out_specs, check_vma=False
    )
```

```python
import functools

import jax
import jax.numpy as jnp
import numpy as np
from jax import lax
from jax.experimental import pallas as pl
from jax.experimental.pallas import tpu as pltpu
from jax.sharding import PartitionSpec as P

HEADS = 16
LAYERS = 2
D = 1024
BLK = 128
NZ = 8
SHARD = 32
WORDS = 384
PO = 256 + D
EPS = 1e-05
MESH = pl.DeviceIdType.MESH
BF = jnp.bfloat16
F32 = jnp.float32


ORDER = (
    ("o", 0), ("o", 1), ("f", 0, 1), ("b", 0, 1), ("y", 0, 0), ("o", 2), ("f", 1, 1),
    ("b", 1, 1), ("f", 0, 2), ("y", 0, 4), ("b", 0, 2), ("y", 0, 1), ("f", 2, 1), ("b", 2, 1),
    ("y", 2, 0), ("f", 1, 2), ("b", 1, 2), ("y", 0, 5), ("f", 0, 3), ("b", 0, 3), ("y", 0, 2),
    ("y", 2, 4), ("f", 2, 2), ("o", 3), ("b", 2, 2), ("y", 2, 1), ("o", 4), ("f", 1, 3),
    ("b", 1, 3), ("f", 0, 4), ("d", 0, 0), ("y", 0, 6), ("y", 0, 3), ("f", 2, 3), ("y", 2, 5),
    ("b", 3, 1), ("y", 3, 0), ("f", 3, 1), ("o", 5), ("b", 2, 3), ("y", 2, 2), ("d", 0, 2),
    ("f", 4, 1), ("b", 4, 1), ("y", 0, 7), ("d", 0, 1), ("f", 1, 4), ("d", 1, 0), ("y", 2, 6),
    ("b", 3, 2), ("f", 2, 4), ("d", 2, 0), ("b", 5, 1), ("y", 3, 4), ("y", 3, 1), ("f", 3, 2),
    ("b", 4, 2), ("y", 5, 0), ("d", 0, 3), ("f", 5, 1), ("b", 3, 3), ("d", 1, 1), ("y", 2, 3),
    ("d", 2, 2), ("f", 4, 2), ("b", 5, 2), ("y", 2, 7), ("d", 2, 1), ("f", 3, 3), ("b", 4, 3),
    ("y", 3, 5), ("c", "q0"), ("y", 3, 2), ("f", 5, 2), ("c", "v0"), ("d", 2, 3), ("f", 4, 3),
    ("b", 5, 3), ("y", 5, 1), ("y", 5, 4), ("f", 3, 4), ("d", 3, 0), ("f", 5, 3), ("y", 3, 6),
    ("c", "a00"), ("y", 3, 3), ("c", "a01"), ("f", 4, 4), ("d", 4, 0), ("y", 5, 2),
    ("y", 5, 5), ("c", "a02"), ("c", "a03"), ("f", 5, 4), ("d", 5, 0), ("t", 0), ("c", "p0"),
    ("y", 3, 7), ("d", 3, 2), ("d", 3, 1), ("y", 5, 3), ("c", "n0"), ("y", 5, 6), ("d", 5, 2),
    ("d", 4, 1), ("y", 5, 7), ("d", 5, 1), ("d", 3, 3), ("d", 5, 3), ("c", "q1"), ("c", "k1"),
    ("c", "m1"), ("c", "a10"), ("c", "a11"), ("c", "a12"), ("c", "a13"), ("c", "p1"), ("t", 1),
    ("c", "n1"),
)


def pos_table_t(row_count, model_width):
    distance = np.arange(row_count - 1, -1, -1).astype(np.float32)
    inverse = np.float32(1.0) / np.float32(10000.0) ** (
        np.arange(0, model_width, 2).astype(np.float32) / np.float32(model_width)
    )
    angles = distance[:, None] * inverse[None, :].astype(np.float32)
    table = np.concatenate([np.sin(angles), np.cos(angles)], axis=1)
    return jnp.asarray(table.T, F32).astype(BF)


def kernel(
    emb, wqkv, w_out, w_pos, ptab, bias_c, bias_p, gain, offset, table, targets, vlen,
    hid_out, tl_out, loss_out,
    W, POW, T, X0, X1, QC, QP, K, V, ATT, Y, HALL, STL, ST, PART, WP, PT,
    lsem, ring_r, y_r, x_r, d_r, w_s, halo_s, halo_r, t_s, t_r, h_s, h_r, st_s, st_r, p_s, p_r,
):
    i = lax.axis_index("seq")
    b = lax.axis_index("batch")
    c = i % 2
    z = (i // 2) % NZ
    y = i // (2 * NZ)
    sgn = 1 - 2 * c

    def dev(yy, zz, cc):
        return (yy * NZ + zz) * 2 + cc

    def zoff(k):
        return (z + 2 * NZ + k) % NZ

    fwd = {"seq": dev(y, zoff(sgn), c)}
    bwd = {"seq": dev(y, zoff(-sgn), c)}
    partner = {"seq": dev(y, z, 1 - c)}
    diag = {"seq": dev(1 - y, z, 1 - c)}
    near = {"seq": dev(1 - y, z, c)}
    far = {"seq": dev(1 - y, z, c), "batch": (b // 2) * 2 + 1 - b % 2}
    nxt = {"seq": (i + 1) % 32}
    prv = {"seq": (i + 31) % 32}
    x = b // 2
    xp = x % 2
    right = {"batch": ((x + 1) % 4) * 2 + b % 2}
    left = {"batch": ((x + 3) % 4) * 2 + b % 2}

    def rcopy(src, dst, ss, rs, to):
        return pltpu.make_async_remote_copy(
            src_ref=src, dst_ref=dst, send_sem=ss, recv_sem=rs, device_id=to, device_id_type=MESH
        )

    loc = [
        pltpu.make_async_copy(wqkv.at[0], W.at[0, y, z, c], lsem.at[0]),
        pltpu.make_async_copy(emb, X0.at[1], lsem.at[1]),
        pltpu.make_async_copy(w_pos, WP, lsem.at[2]),
        pltpu.make_async_copy(ptab, PT, lsem.at[3]),
        pltpu.make_async_copy(w_out, POW.at[:, y, z, c, :, pl.ds(256, D)], lsem.at[4]),
        pltpu.make_async_copy(wqkv.at[1], W.at[1, y, z, c], lsem.at[5]),
        pltpu.make_async_copy(table, T.at[y, c], lsem.at[6]),
    ]
    for cp in loc:
        cp.start()

    barrier = pltpu.get_barrier_semaphore()
    for k in range(1, NZ):
        pl.semaphore_signal(barrier, inc=1, device_id={"seq": dev(y, zoff(k), c)}, device_id_type=MESH)
    for peer in (partner, diag, near, far, nxt, prv, right, left):
        pl.semaphore_signal(barrier, inc=1, device_id=peer, device_id_type=MESH)
    pl.semaphore_wait(barrier, NZ - 1 + 8)

    def piece(si, yy, zz, kind):
        layer, part = si // 3, si % 3
        if part == 2:
            at, size = {"ring": (xp * 384, 896), "give": (xp * 896, 384), "take": ((1 - xp) * 896, 384)}[kind]
            return POW.at[layer, yy, zz, c, :, pl.ds(pl.multiple_of(at, 128), size)]
        if part == 1:
            return W.at[layer, yy, zz, c, :, pl.ds(D, D)]
        at = (1 - xp if kind == "take" else xp) * 2 * D
        return W.at[layer, yy, zz, c, :, pl.ds(pl.multiple_of(at, D), D)]

    def shares(si):
        return si % 3 != 1

    def place(k):
        return zoff(sgn * k) if k < 4 else zoff(-sgn * (k - 3))

    def ring_copy(si, zz, to, k):
        s = piece(si, y, zz, "ring")
        return rcopy(s, s, w_s.at[si, 0 if k < 4 else 1], ring_r.at[si, k], to)

    def y_copy(si, k):
        s = piece(si, y, place(k), "ring")
        slot = k if shares(si) else k // 4 * 4
        return rcopy(s, s, w_s.at[si, 2 + k // 4], y_r.at[si, slot], far if k >= 4 else near)

    def x_copy(si, yy, k, other):
        s = piece(si, yy, place(k), "give")
        return rcopy(s, s, w_s.at[si, 4 + k // 4], x_r.at[si, 2 * other + k // 4], left if k >= 4 else right)

    def d_copy(si, n):
        s = piece(si, y if n % 2 == 0 else 1 - y, pl.ds(0, NZ), "ring" if n < 2 else "take")
        return rcopy(s, s, w_s.at[si, 6 + n], d_r.at[si, n], partner)

    def several(si, kind, recv, n=4):
        s = piece(si, y, pl.ds(0, n), kind)
        return rcopy(s, s, w_s.at[si, 0], recv, partner)

    def own(si):
        ring_copy(si, z, fwd, 0).start()
        ring_copy(si, z, bwd, 4).start()
        y_copy(si, 0).start()

    def forward(si, d):
        zz = zoff(-sgn * d)
        ring_copy(si, zz, fwd, d - 1).wait_recv()
        if d < 4:
            ring_copy(si, zz, fwd, d).start()
        y_copy(si, 3 + d).start()
        if shares(si):
            x_copy(si, y, 3 + d, 0).start()

    def backward(si, d):
        zz = zoff(sgn * d)
        ring_copy(si, zz, bwd, 3 + d).wait_recv()
        if d < 3:
            ring_copy(si, zz, bwd, 4 + d).start()
        y_copy(si, d).start()
        if shares(si):
            x_copy(si, y, d, 0).start()

    def across(si, k):
        y_copy(si, k).wait_recv()
        x_copy(si, 1 - y, k, 1).start()

    def to_partner(si, n):
        if n == 1 and not shares(si):
            several(si, "ring", y_r.at[si, 0]).wait_recv()
            several(si, "ring", y_r.at[si, 4]).wait_recv()
        if n >= 2:
            several(si, "take", x_r.at[si, 2 * n - 4], n + 1).wait_recv()
            several(si, "take", x_r.at[si, 2 * n - 3]).wait_recv()
        d_copy(si, n).start()

    def finish(si):
        for n in range(4 if shares(si) else 2):
            d_copy(si, n).wait_recv()

    def drain(si):
        waits = [("ring", 0, 4), ("ring", 1, 3), ("ring", 2, 4), ("ring", 3, 4), ("ring", 6, 8), ("ring", 7, 8)]
        if shares(si):
            waits += [("give", 4, 7), ("give", 5, 8), ("take", 8, 8), ("take", 9, 8)]
        for kind, k, n in waits:
            s = piece(si, y, pl.ds(0, n), kind)
            rcopy(s, s, w_s.at[si, k], ring_r.at[si, 0], fwd).wait_send()

    low = lax.broadcasted_iota(jnp.int32, (BLK, BLK), 1) < 64
    rows = lax.broadcasted_iota(jnp.int32, (BLK, 2 * BLK), 0)
    cols = lax.broadcasted_iota(jnp.int32, (BLK, 2 * BLK), 1)
    first_key = BLK * (1 - jnp.minimum(i, 1))
    allowed = (cols <= rows + BLK) & (cols >= first_key)

    def lanes(t, size):
        return pl.ds(pl.multiple_of(t * size, size), size)

    def weights(layer, col):
        return W[layer, :, :, :, :, pl.ds(pl.multiple_of(col, 256), 256)].reshape(D, 256)

    def queries(layer, X):
        def body(t, carry):
            sl = lanes(t, 256)
            q = jnp.dot(X[1], weights(layer, t * 256), preferred_element_type=F32)
            QC[:, sl] = (q + bias_c[layer : layer + 1, sl]).astype(BF)
            QP[:, sl] = (q + bias_p[layer : layer + 1, sl]).astype(BF)
            return carry

        lax.fori_loop(0, 4, body, 0)

    def keys_values(layer, X, part):
        row0, count = {"all": (0, 2), "own": (1, 1), "memory": (0, 1)}[part]

        def body(t, carry):
            x = X[row0 : row0 + count].reshape(count * BLK, D)
            r = pl.ds(row0 * BLK, count * BLK)
            sl = lanes(t, 256)
            K[r, sl] = jnp.dot(x, weights(layer, D + t * 256), preferred_element_type=F32).astype(BF)
            V[r, sl] = jnp.dot(x, weights(layer, 2 * D + t * 256), preferred_element_type=F32).astype(BF)
            return carry

        lax.fori_loop(0, 4, body, 0)

    def both(x):
        zero = jnp.zeros_like(x)
        return jnp.concatenate([jnp.where(low, x, zero), jnp.where(low, zero, x)], 0)

    def attend(layer, start, stop):
        def body(p, carry):
            sl = lanes(p, BLK)
            q2 = both(QC[:, sl].astype(F32)).astype(BF)
            r2 = both(QP[:, sl].astype(F32)).astype(BF)
            content = lax.dot_general(
                q2, K[:, sl], (((1,), (1,)), ((), ())), preferred_element_type=F32
            )
            pos = POW[layer, p // 4, pl.ds((p % 4) * 2, 2), :, :, 0:256].reshape(BLK, 2 * BLK)
            position = jnp.dot(r2, pos, preferred_element_type=F32)
            outs = []
            for k in range(2):
                half = slice(k * BLK, (k + 1) * BLK)
                shifted = pltpu.roll(position[half], BLK + 1, 1, stride=1, stride_axis=0)
                scores = (content[half] + shifted) * 0.125
                e = jnp.where(allowed, jnp.exp(scores), 0.0)
                outs.append((e / jnp.sum(e, -1, keepdims=True)).astype(BF))
            o = jnp.dot(jnp.concatenate(outs, 0), V[:, sl], preferred_element_type=F32)
            ATT[:, sl] = jnp.where(low, o[:BLK], o[BLK:]).astype(BF)
            return carry

        lax.fori_loop(start, stop, body, 0)

    def project(layer, X):
        def body(t, carry):
            sl = lanes(t, 256)
            w = POW[layer, :, :, :, :, pl.ds(pl.multiple_of(256 + t * 256, 256), 256)].reshape(D, 256)
            Y[:, sl] = jnp.dot(ATT[...], w, preferred_element_type=F32) + X[1, :, sl].astype(F32)
            return carry

        lax.fori_loop(0, 4, body, 0)

    def norm(layer, dst, last):
        def body(t, carry):
            r = pl.ds(pl.multiple_of(t * 32, 32), 32)
            v = Y[r, :]
            v = v - jnp.mean(v, -1, keepdims=True)
            spread = jnp.mean(v * v, -1, keepdims=True)
            h = v * lax.rsqrt(spread + EPS) * gain[layer : layer + 1, :] + offset[layer : layer + 1, :]
            dst[r, :] = h.astype(BF)
            if last:
                pos = lax.broadcasted_iota(jnp.int32, (32, D), 0) + (i * BLK + t * 32)
                hid_out[r, :] = jnp.where(pos < vlen[0], h, 0.0).astype(BF)
            return carry

        lax.fori_loop(0, 4, body, 0)

    halves = (pl.ds(0, WORDS // 2), pl.ds(WORDS // 2, WORDS // 2))
    tcopies = [
        rcopy(T.at[y, c, h], T.at[y, c, h], t_s.at[k], t_r.at[k], to)
        for k, (h, to) in enumerate(zip(halves, (near, far)))
    ] + [rcopy(T.at[y, c], T.at[y, c], t_s.at[2], t_r.at[2], partner)]
    t_other = rcopy(T.at[1 - y, c], T.at[1 - y, c], t_s.at[3], t_r.at[3], partner)
    halo0 = rcopy(X0.at[1], X0.at[0], halo_s.at[0], halo_r.at[0], nxt)
    halo1 = rcopy(X1.at[1], X1.at[0], halo_s.at[1], halo_r.at[1], nxt)

    def table_step(n):
        if n == 0:
            for cp in tcopies:
                cp.start()
        else:
            tcopies[0].wait_recv()
            tcopies[1].wait_recv()
            t_other.start()

    def compute(name):
        kind, layer = name[0], int(name[1])
        X = (X0, X1)[layer]
        if name == "q0":
            finish(0)
            finish(1)
            queries(0, X0)
        elif name == "v0":
            halo0.wait_recv()
            keys_values(0, X0, "all")
        elif name == "q1":
            finish(3)
            finish(4)
            queries(1, X1)
        elif name == "k1":
            keys_values(1, X1, "own")
        elif name == "m1":
            halo1.wait_recv()
            keys_values(1, X1, "memory")
        elif kind == "a":
            k = int(name[2])
            if k == 0:
                finish(2 + 3 * layer)
            attend(layer, 2 * k, 2 * k + 2)
        elif kind == "p":
            project(layer, X)
        elif name == "n0":
            norm(0, X1.at[1], False)
            halo1.start()
        else:
            norm(1, HALL.at[0], True)

    def start_rest():
        loc[1].wait()
        halo0.start()
        loc[2].wait()
        loc[3].wait()
        for layer in range(LAYERS):
            share = lax.dot_general(
                WP[layer], PT[...], (((0,), (0,)), ((), ())), preferred_element_type=F32
            )
            POW[layer, y, z, c, :, 0:256] = share.astype(BF)
        for cp in loc[4:]:
            cp.wait()

    handlers = {"o": own, "f": forward, "b": backward, "y": across, "d": to_partner, "t": table_step}
    loc[0].wait()
    for n, (kind, *at) in enumerate(ORDER):
        if kind == "c":
            compute(at[0])
        else:
            handlers[kind](*at)
        if n == 1:
            start_rest()

    hv = (pl.ds(0, BLK // 2), pl.ds(BLK // 2, BLK // 2))

    def hcopy(d, backward, half):
        src = 0 if d == 0 else (2 * d if backward else 2 * d - 1)
        dst = 2 * d + 2 if backward else 2 * d + 1
        k = (4 if backward else 0) + d
        return rcopy(
            HALL.at[src, hv[half]], HALL.at[dst, hv[half]],
            h_s.at[1 if backward else 0], h_r.at[k, half], bwd if backward else fwd,
        )

    for half in (0, 1):
        hcopy(0, False, half).start()
        hcopy(0, True, half).start()

    tcopies[2].wait_recv()
    t_other.wait_recv()

    def stats(slot, blocks):
        n = len(blocks)
        hb = HALL[slot : slot + n].reshape(n * BLK, D)
        tg = [targets[pl.ds(dev(y, zz, c), 1), :] for zz in blocks]
        tg = tg[0] if n == 1 else jnp.concatenate(tg, 1)
        word = lax.broadcasted_iota(jnp.int32, (WORDS, n * BLK), 0)

        def body(k, carry):
            sums, picks = carry
            first = dev(k // 2, z, k % 2) * WORDS
            logits = lax.dot_general(
                T[k // 2, k % 2], hb, (((1,), (1,)), ((), ())), preferred_element_type=F32
            )
            sums = sums + jnp.sum(jnp.exp(logits), 0, keepdims=True)
            picks = picks + jnp.sum(jnp.where(word == tg - first, logits, 0.0), 0, keepdims=True)
            return sums, picks

        zero = jnp.zeros((1, n * BLK), F32)
        sums, picks = lax.fori_loop(0, 4, body, (zero, zero))
        for k, zz in enumerate(blocks):
            STL[pl.ds(zz, 1), :] = sums[:, k * BLK : (k + 1) * BLK]
            STL[pl.ds(NZ + zz, 1), :] = picks[:, k * BLK : (k + 1) * BLK]

    stats(0, [z])
    for d in (1, 2, 3, 4):
        for half in (0, 1):
            hcopy(d - 1, False, half).wait_recv()
            if d < 4:
                hcopy(d, False, half).start()
                hcopy(d - 1, True, half).wait_recv()
                if d < 3:
                    hcopy(d, True, half).start()
        if d < 4:
            stats(2 * d - 1, [zoff(-sgn * d), zoff(sgn * d)])
        else:
            stats(7, [zoff(4)])

    scopies = []
    for k in range(1, NZ):
        cp = rcopy(STL, ST.at[k], st_s.at[k - 1], st_r.at[k - 1], {"seq": dev(y, zoff(k), c)})
        cp.start()
        scopies.append(cp)
    ST[0] = STL[...]
    for cp in scopies:
        cp.wait_recv()

    def add(k, total):
        return total + ST[(z + 2 * NZ - k) % NZ]

    total = lax.fori_loop(0, NZ, add, jnp.zeros((2 * NZ, BLK), F32))
    token = lax.broadcasted_iota(jnp.int32, (NZ, BLK), 0) * (2 * BLK) + (
        lax.broadcasted_iota(jnp.int32, (NZ, BLK), 1) + (y * NZ * 2 + c) * BLK
    )
    per_token = jnp.where(token < vlen[0], jnp.log(total[:NZ]) - total[NZ:], 0.0)
    mine = lax.broadcasted_iota(jnp.int32, (NZ, BLK), 0) == z
    tl_out[...] = jnp.sum(jnp.where(mine, per_token, 0.0), 0, keepdims=True)
    PART[pl.ds(2 * y + c, 1)] = per_token[None]
    pc = []
    for k, to in enumerate((partner, near, diag)):
        s = PART.at[2 * y + c]
        cp = rcopy(s, s, p_s.at[k], p_r.at[k], to)
        cp.start()
        pc.append(cp)
    for cp in pc:
        cp.wait_recv()
    loss = jnp.sum(PART[0] + PART[1] + (PART[2] + PART[3])) / vlen[0].astype(F32)
    loss_out[...] = jnp.full((1, BLK), loss, F32)

    for cp in pc + scopies:
        cp.wait_send()
    for si in range(6):
        drain(si)
    halo0.wait_send()
    halo1.wait_send()
    for cp in tcopies + [t_other]:
        cp.wait_send()
    for k, n in ((0, 4), (1, 3)):
        s = HALL.at[pl.ds(0, n)]
        rcopy(s, s, h_s.at[k], h_r.at[0, 0], fwd).wait_send()


def on_device(
    embedded, w_qkv, w_out, w_pos, bias_content, bias_position, norm_gain, norm_offset,
    table, targets, valid_length,
):
    vmem = pl.BlockSpec(memory_space=pltpu.VMEM)
    hbm = pl.BlockSpec(memory_space=pl.ANY)
    smem = pl.BlockSpec(memory_space=pltpu.SMEM)
    DMA = pltpu.SemaphoreType.DMA
    hidden, token_loss, loss = pl.pallas_call(
        kernel,
        out_shape=(
            jax.ShapeDtypeStruct((BLK, D), BF),
            jax.ShapeDtypeStruct((1, BLK), F32),
            jax.ShapeDtypeStruct((1, BLK), F32),
        ),
        in_specs=[hbm] * 5 + [vmem] * 4 + [hbm, vmem, smem],
        out_specs=(vmem, vmem, vmem),
        scratch_shapes=[
            pltpu.VMEM((LAYERS, 2, NZ, 2, SHARD, 3 * D), BF),
            pltpu.VMEM((LAYERS, 2, NZ, 2, SHARD, PO), BF),
            pltpu.VMEM((2, 2, WORDS, D), BF),
            pltpu.VMEM((2, BLK, D), BF),
            pltpu.VMEM((2, BLK, D), BF),
            pltpu.VMEM((BLK, D), BF),
            pltpu.VMEM((BLK, D), BF),
            pltpu.VMEM((2 * BLK, D), BF),
            pltpu.VMEM((2 * BLK, D), BF),
            pltpu.VMEM((BLK, D), BF),
            pltpu.VMEM((BLK, D), F32),
            pltpu.VMEM((NZ, BLK, D), BF),
            pltpu.VMEM((2 * NZ, BLK), F32),
            pltpu.VMEM((NZ, 2 * NZ, BLK), F32),
            pltpu.VMEM((4, NZ, BLK), F32),
            pltpu.VMEM((LAYERS, D, SHARD), BF),
            pltpu.VMEM((D, 2 * BLK), BF),
            DMA((7,)),
            DMA((6, 7)),
            DMA((6, 8)),
            DMA((6, 4)),
            DMA((6, 4)),
            DMA((6, 10)),
            DMA((2,)),
            DMA((2,)),
            DMA((4,)),
            DMA((4,)),
            DMA((2,)),
            DMA((7, 2)),
            DMA((NZ - 1,)),
            DMA((NZ - 1,)),
            DMA((3,)),
            DMA((3,)),
        ],
        compiler_params=pltpu.CompilerParams(
            collective_id=0, has_side_effects=True, vmem_limit_bytes=58 * 1024 * 1024
        ),
    )(
        embedded, w_qkv, w_out, w_pos, pos_table_t(2 * BLK, D), bias_content, bias_position, norm_gain, norm_offset,
        table, targets.reshape(32, BLK), valid_length,
    )
    return hidden, token_loss.reshape(BLK), loss[0, :1]


def solution(mesh):
    in_specs = (
        P(("batch", "seq"), None),
        P(None, "seq", None),
        P(None, "seq", None),
        P(None, None, "seq"),
        P(),
        P(),
        P(),
        P(),
        P("seq", None),
        P("batch"),
        P("batch"),
    )
    out_specs = (P(("batch", "seq"), None), P(("batch", "seq")), P("batch"))
    return jax.shard_map(
        on_device, mesh=mesh, in_specs=in_specs, out_specs=out_specs, check_vma=False
    )
```

```python
import functools

import jax
import jax.numpy as jnp
import numpy as np
from jax import lax
from jax.experimental import pallas as pl
from jax.experimental.pallas import tpu as pltpu
from jax.sharding import PartitionSpec as P

HEADS = 16
LAYERS = 2
D = 1024
BLK = 128
NZ = 8
SHARD = 32
WORDS = 384
PO = 256 + D
EPS = 1e-05
MESH = pl.DeviceIdType.MESH
BF = jnp.bfloat16
F32 = jnp.float32


ORDER = (
    ("o", 0), ("o", 1), ("o", 2), ("f", 0, 1), ("b", 0, 1), ("y", 0, 0), ("f", 1, 1),
    ("b", 1, 1), ("f", 2, 1), ("b", 2, 1), ("y", 2, 0), ("y", 0, 4), ("f", 0, 2), ("b", 0, 2),
    ("y", 0, 1), ("f", 1, 2), ("b", 1, 2), ("y", 2, 4), ("f", 2, 2), ("b", 2, 2), ("y", 2, 1),
    ("y", 0, 5), ("f", 0, 3), ("b", 0, 3), ("y", 0, 2), ("o", 3), ("f", 1, 3), ("b", 1, 3),
    ("y", 2, 5), ("f", 2, 3), ("b", 2, 3), ("y", 2, 2), ("y", 0, 6), ("f", 0, 4), ("y", 0, 3),
    ("d", 0, 0), ("b", 3, 1), ("f", 3, 1), ("o", 4), ("o", 5), ("f", 1, 4), ("d", 1, 0),
    ("y", 3, 0), ("f", 2, 4), ("d", 2, 0), ("y", 2, 6), ("b", 3, 2), ("y", 0, 7), ("d", 0, 1),
    ("y", 2, 3), ("f", 3, 2), ("b", 4, 1), ("d", 0, 2), ("y", 3, 4), ("y", 3, 1), ("b", 5, 1),
    ("f", 4, 1), ("d", 1, 1), ("d", 2, 2), ("f", 5, 1), ("b", 3, 3), ("y", 2, 7), ("d", 2, 1),
    ("y", 5, 0), ("f", 3, 3), ("d", 0, 3), ("b", 4, 2), ("y", 3, 5), ("y", 3, 2), ("b", 5, 2),
    ("f", 4, 2), ("f", 5, 2), ("c", "q0"), ("c", "v0"), ("f", 3, 4), ("d", 3, 0), ("d", 2, 3),
    ("b", 4, 3), ("y", 5, 1), ("y", 5, 4), ("y", 3, 6), ("b", 5, 3), ("f", 4, 3), ("y", 3, 3),
    ("f", 5, 3), ("c", "a00"), ("c", "a01"), ("y", 5, 5), ("c", "a02"), ("f", 4, 4),
    ("d", 4, 0), ("y", 5, 2), ("c", "a03"), ("y", 3, 7), ("d", 3, 2), ("d", 3, 1), ("f", 5, 4),
    ("d", 5, 0), ("t", 0), ("c", "p0"), ("c", "n0"), ("y", 5, 3), ("y", 5, 6), ("d", 4, 1),
    ("d", 3, 3), ("d", 5, 2), ("y", 5, 7), ("d", 5, 1), ("c", "q1"), ("c", "k1"), ("d", 5, 3),
    ("c", "m1"), ("c", "a10"), ("c", "a11"), ("c", "a12"), ("c", "a13"), ("c", "p1"),
    ("c", "n1"), ("t", 1),
)


def pos_table_t(row_count, model_width):
    distance = np.arange(row_count - 1, -1, -1).astype(np.float32)
    inverse = np.float32(1.0) / np.float32(10000.0) ** (
        np.arange(0, model_width, 2).astype(np.float32) / np.float32(model_width)
    )
    angles = distance[:, None] * inverse[None, :].astype(np.float32)
    table = np.concatenate([np.sin(angles), np.cos(angles)], axis=1)
    return jnp.asarray(table.T, F32).astype(BF)


def kernel(
    emb, wqkv, w_out, w_pos, ptab, bias_c, bias_p, gain, offset, table, targets, vlen,
    hid_out, tl_out, loss_out,
    W, POW, T, X0, X1, QC, QP, K, V, ATT, Y, HALL, STL, ST, PART, WP, PT,
    lsem, ring_r, y_r, x_r, d_r, w_s, halo_s, halo_r, t_s, t_r, h_s, h_r, st_s, st_r, p_s, p_r,
):
    i = lax.axis_index("seq")
    b = lax.axis_index("batch")
    c = i % 2
    z = (i // 2) % NZ
    y = i // (2 * NZ)
    sgn = 1 - 2 * c

    def dev(yy, zz, cc):
        return (yy * NZ + zz) * 2 + cc

    def zoff(k):
        return (z + 2 * NZ + k) % NZ

    fwd = {"seq": dev(y, zoff(sgn), c)}
    bwd = {"seq": dev(y, zoff(-sgn), c)}
    partner = {"seq": dev(y, z, 1 - c)}
    diag = {"seq": dev(1 - y, z, 1 - c)}
    near = {"seq": dev(1 - y, z, c)}
    far = {"seq": dev(1 - y, z, c), "batch": (b // 2) * 2 + 1 - b % 2}
    nxt = {"seq": (i + 1) % 32}
    prv = {"seq": (i + 31) % 32}
    x = b // 2
    xp = x % 2
    right = {"batch": ((x + 1) % 4) * 2 + b % 2}
    left = {"batch": ((x + 3) % 4) * 2 + b % 2}

    def rcopy(src, dst, ss, rs, to):
        return pltpu.make_async_remote_copy(
            src_ref=src, dst_ref=dst, send_sem=ss, recv_sem=rs, device_id=to, device_id_type=MESH
        )

    loc = [
        pltpu.make_async_copy(wqkv.at[0], W.at[0, y, z, c], lsem.at[0]),
        pltpu.make_async_copy(emb, X0.at[1], lsem.at[1]),
        pltpu.make_async_copy(w_pos, WP, lsem.at[2]),
        pltpu.make_async_copy(ptab, PT, lsem.at[3]),
        pltpu.make_async_copy(w_out, POW.at[:, y, z, c, :, pl.ds(256, D)], lsem.at[4]),
        pltpu.make_async_copy(wqkv.at[1], W.at[1, y, z, c], lsem.at[5]),
        pltpu.make_async_copy(table, T.at[y, c], lsem.at[6]),
    ]
    for cp in loc:
        cp.start()

    barrier = pltpu.get_barrier_semaphore()
    for peer in (fwd, bwd, partner, diag, near, far, nxt, prv, right, left):
        pl.semaphore_signal(barrier, inc=1, device_id=peer, device_id_type=MESH)
    pl.semaphore_wait(barrier, 10)

    def piece(si, yy, zz, kind):
        layer, part = si // 3, si % 3
        if part == 2:
            at, size = {"ring": (xp * 384, 896), "give": (xp * 896, 384), "take": ((1 - xp) * 896, 384)}[kind]
            return POW.at[layer, yy, zz, c, :, pl.ds(pl.multiple_of(at, 128), size)]
        if part == 1:
            return W.at[layer, yy, zz, c, :, pl.ds(D, D)]
        at = (1 - xp if kind == "take" else xp) * 2 * D
        return W.at[layer, yy, zz, c, :, pl.ds(pl.multiple_of(at, D), D)]

    def shares(si):
        return si % 3 != 1

    def place(k):
        return zoff(sgn * k) if k < 4 else zoff(-sgn * (k - 3))

    def ring_copy(si, zz, to, k):
        s = piece(si, y, zz, "ring")
        return rcopy(s, s, w_s.at[si, 0 if k < 4 else 1], ring_r.at[si, k], to)

    def y_copy(si, k):
        s = piece(si, y, place(k), "ring")
        slot = k if shares(si) else k // 4 * 4
        return rcopy(s, s, w_s.at[si, 2 + k // 4], y_r.at[si, slot], far if k >= 4 else near)

    def x_copy(si, yy, k, other):
        s = piece(si, yy, place(k), "give")
        return rcopy(s, s, w_s.at[si, 4 + k // 4], x_r.at[si, 2 * other + k // 4], left if k >= 4 else right)

    def d_copy(si, n):
        s = piece(si, y if n % 2 == 0 else 1 - y, pl.ds(0, NZ), "ring" if n < 2 else "take")
        return rcopy(s, s, w_s.at[si, 6 + n], d_r.at[si, n], partner)

    def several(si, kind, recv, n=4):
        s = piece(si, y, pl.ds(0, n), kind)
        return rcopy(s, s, w_s.at[si, 0], recv, partner)

    def own(si):
        ring_copy(si, z, fwd, 0).start()
        ring_copy(si, z, bwd, 4).start()
        y_copy(si, 0).start()

    def forward(si, d):
        zz = zoff(-sgn * d)
        ring_copy(si, zz, fwd, d - 1).wait_recv()
        if d < 4:
            ring_copy(si, zz, fwd, d).start()
        y_copy(si, 3 + d).start()
        if shares(si):
            x_copy(si, y, 3 + d, 0).start()

    def backward(si, d):
        zz = zoff(sgn * d)
        ring_copy(si, zz, bwd, 3 + d).wait_recv()
        if d < 3:
            ring_copy(si, zz, bwd, 4 + d).start()
        y_copy(si, d).start()
        if shares(si):
            x_copy(si, y, d, 0).start()

    def across(si, k):
        y_copy(si, k).wait_recv()
        x_copy(si, 1 - y, k, 1).start()

    def to_partner(si, n):
        if n == 1 and not shares(si):
            several(si, "ring", y_r.at[si, 0]).wait_recv()
            several(si, "ring", y_r.at[si, 4]).wait_recv()
        if n >= 2:
            several(si, "take", x_r.at[si, 2 * n - 4], n + 1).wait_recv()
            several(si, "take", x_r.at[si, 2 * n - 3]).wait_recv()
        d_copy(si, n).start()

    def finish(si):
        for n in range(4 if shares(si) else 2):
            d_copy(si, n).wait_recv()

    def drain(si):
        waits = [("ring", 0, 4), ("ring", 1, 3), ("ring", 2, 4), ("ring", 3, 4), ("ring", 6, 8), ("ring", 7, 8)]
        if shares(si):
            waits += [("give", 4, 7), ("give", 5, 8), ("take", 8, 8), ("take", 9, 8)]
        for kind, k, n in waits:
            s = piece(si, y, pl.ds(0, n), kind)
            rcopy(s, s, w_s.at[si, k], ring_r.at[si, 0], fwd).wait_send()

    low = lax.broadcasted_iota(jnp.int32, (BLK, BLK), 1) < 64
    rows = lax.broadcasted_iota(jnp.int32, (BLK, 2 * BLK), 0)
    cols = lax.broadcasted_iota(jnp.int32, (BLK, 2 * BLK), 1)
    first_key = BLK * (1 - jnp.minimum(i, 1))
    allowed = (cols <= rows + BLK) & (cols >= first_key)

    def lanes(t, size):
        return pl.ds(pl.multiple_of(t * size, size), size)

    def weights(layer, col):
        return W[layer, :, :, :, :, pl.ds(pl.multiple_of(col, 256), 256)].reshape(D, 256)

    def queries(layer, X):
        def body(t, carry):
            sl = lanes(t, 256)
            q = jnp.dot(X[1], weights(layer, t * 256), preferred_element_type=F32)
            QC[:, sl] = (q + bias_c[layer : layer + 1, sl]).astype(BF)
            QP[:, sl] = (q + bias_p[layer : layer + 1, sl]).astype(BF)
            return carry

        lax.fori_loop(0, 4, body, 0)

    def keys_values(layer, X, part):
        row0, count = {"all": (0, 2), "own": (1, 1), "memory": (0, 1)}[part]

        def body(t, carry):
            x = X[row0 : row0 + count].reshape(count * BLK, D)
            r = pl.ds(row0 * BLK, count * BLK)
            sl = lanes(t, 256)
            K[r, sl] = jnp.dot(x, weights(layer, D + t * 256), preferred_element_type=F32).astype(BF)
            V[r, sl] = jnp.dot(x, weights(layer, 2 * D + t * 256), preferred_element_type=F32).astype(BF)
            return carry

        lax.fori_loop(0, 4, body, 0)

    def both(x):
        zero = jnp.zeros_like(x)
        return jnp.concatenate([jnp.where(low, x, zero), jnp.where(low, zero, x)], 0)

    def attend(layer, start, stop):
        def body(p, carry):
            sl = lanes(p, BLK)
            q2 = both(QC[:, sl].astype(F32)).astype(BF)
            r2 = both(QP[:, sl].astype(F32)).astype(BF)
            content = lax.dot_general(
                q2, K[:, sl], (((1,), (1,)), ((), ())), preferred_element_type=F32
            )
            pos = POW[layer, p // 4, pl.ds((p % 4) * 2, 2), :, :, 0:256].reshape(BLK, 2 * BLK)
            position = jnp.dot(r2, pos, preferred_element_type=F32)
            outs = []
            for k in range(2):
                half = slice(k * BLK, (k + 1) * BLK)
                shifted = pltpu.roll(position[half], BLK + 1, 1, stride=1, stride_axis=0)
                scores = (content[half] + shifted) * 0.125
                e = jnp.where(allowed, jnp.exp(scores), 0.0)
                outs.append((e / jnp.sum(e, -1, keepdims=True)).astype(BF))
            o = jnp.dot(jnp.concatenate(outs, 0), V[:, sl], preferred_element_type=F32)
            ATT[:, sl] = jnp.where(low, o[:BLK], o[BLK:]).astype(BF)
            return carry

        lax.fori_loop(start, stop, body, 0)

    def project(layer, X):
        def body(t, carry):
            sl = lanes(t, 256)
            w = POW[layer, :, :, :, :, pl.ds(pl.multiple_of(256 + t * 256, 256), 256)].reshape(D, 256)
            Y[:, sl] = jnp.dot(ATT[...], w, preferred_element_type=F32) + X[1, :, sl].astype(F32)
            return carry

        lax.fori_loop(0, 4, body, 0)

    def norm(layer, dst, last):
        def body(t, carry):
            r = pl.ds(pl.multiple_of(t * 32, 32), 32)
            v = Y[r, :]
            v = v - jnp.mean(v, -1, keepdims=True)
            spread = jnp.mean(v * v, -1, keepdims=True)
            h = v * lax.rsqrt(spread + EPS) * gain[layer : layer + 1, :] + offset[layer : layer + 1, :]
            dst[r, :] = h.astype(BF)
            if last:
                pos = lax.broadcasted_iota(jnp.int32, (32, D), 0) + (i * BLK + t * 32)
                hid_out[r, :] = jnp.where(pos < vlen[0], h, 0.0).astype(BF)
            return carry

        lax.fori_loop(0, 4, body, 0)

    halves = (pl.ds(0, WORDS // 2), pl.ds(WORDS // 2, WORDS // 2))
    tcopies = [
        rcopy(T.at[y, c, h], T.at[y, c, h], t_s.at[k], t_r.at[k], to)
        for k, (h, to) in enumerate(zip(halves, (near, far)))
    ] + [rcopy(T.at[y, c], T.at[y, c], t_s.at[2], t_r.at[2], partner)]
    t_other = rcopy(T.at[1 - y, c], T.at[1 - y, c], t_s.at[3], t_r.at[3], partner)
    halo0 = rcopy(X0.at[1], X0.at[0], halo_s.at[0], halo_r.at[0], nxt)
    halo1 = rcopy(X1.at[1], X1.at[0], halo_s.at[1], halo_r.at[1], nxt)

    def table_step(n):
        if n == 0:
            for cp in tcopies:
                cp.start()
        else:
            tcopies[0].wait_recv()
            tcopies[1].wait_recv()
            t_other.start()

    def compute(name):
        kind, layer = name[0], int(name[1])
        X = (X0, X1)[layer]
        if name == "q0":
            finish(0)
            finish(1)
            queries(0, X0)
        elif name == "v0":
            halo0.wait_recv()
            keys_values(0, X0, "all")
        elif name == "q1":
            finish(3)
            finish(4)
            queries(1, X1)
        elif name == "k1":
            keys_values(1, X1, "own")
        elif name == "m1":
            halo1.wait_recv()
            keys_values(1, X1, "memory")
        elif kind == "a":
            k = int(name[2])
            if k == 0:
                finish(2 + 3 * layer)
            attend(layer, 2 * k, 2 * k + 2)
        elif kind == "p":
            project(layer, X)
        elif name == "n0":
            norm(0, X1.at[1], False)
            halo1.start()
        else:
            norm(1, HALL.at[0], True)

    def start_rest():
        loc[1].wait()
        loc[2].wait()
        loc[3].wait()
        for layer in range(LAYERS):
            share = lax.dot_general(
                WP[layer], PT[...], (((1,), (0,)), ((), ())), preferred_element_type=F32
            )
            POW[layer, y, z, c, :, 0:256] = share.astype(BF)
        for cp in loc[4:]:
            cp.wait()

    handlers = {"o": own, "f": forward, "b": backward, "y": across, "d": to_partner, "t": table_step}
    loc[0].wait()
    for n, (kind, *at) in enumerate(ORDER):
        if kind == "c":
            compute(at[0])
        else:
            handlers[kind](*at)
        if n == 1:
            start_rest()
        if ORDER[n] == ("f", 1, 4):
            halo0.start()

    hv = (pl.ds(0, BLK // 2), pl.ds(BLK // 2, BLK // 2))

    def hcopy(d, backward, half):
        src = 0 if d == 0 else (2 * d if backward else 2 * d - 1)
        dst = 2 * d + 2 if backward else 2 * d + 1
        k = (4 if backward else 0) + d
        return rcopy(
            HALL.at[src, hv[half]], HALL.at[dst, hv[half]],
            h_s.at[1 if backward else 0], h_r.at[k, half], bwd if backward else fwd,
        )

    for half in (0, 1):
        hcopy(0, False, half).start()
        hcopy(0, True, half).start()

    tcopies[2].wait_recv()
    t_other.wait_recv()

    def stats(slot, blocks):
        n = len(blocks)
        hb = HALL[slot : slot + n].reshape(n * BLK, D)
        tg = [targets[pl.ds(dev(y, zz, c), 1), :] for zz in blocks]
        tg = tg[0] if n == 1 else jnp.concatenate(tg, 1)
        word = lax.broadcasted_iota(jnp.int32, (WORDS, n * BLK), 0)

        def body(k, carry):
            sums, picks = carry
            first = dev(k // 2, z, k % 2) * WORDS
            logits = lax.dot_general(
                T[k // 2, k % 2], hb, (((1,), (1,)), ((), ())), preferred_element_type=F32
            )
            sums = sums + jnp.sum(jnp.exp(logits), 0, keepdims=True)
            picks = picks + jnp.sum(jnp.where(word == tg - first, logits, 0.0), 0, keepdims=True)
            return sums, picks

        zero = jnp.zeros((1, n * BLK), F32)
        sums, picks = lax.fori_loop(0, 4, body, (zero, zero))
        for k, zz in enumerate(blocks):
            STL[pl.ds(zz, 1), :] = sums[:, k * BLK : (k + 1) * BLK]
            STL[pl.ds(NZ + zz, 1), :] = picks[:, k * BLK : (k + 1) * BLK]

    stats(0, [z])
    for d in (1, 2, 3, 4):
        for half in (0, 1):
            hcopy(d - 1, False, half).wait_recv()
            if d < 4:
                hcopy(d, False, half).start()
                hcopy(d - 1, True, half).wait_recv()
                if d < 3:
                    hcopy(d, True, half).start()
        if d < 4:
            stats(2 * d - 1, [zoff(-sgn * d), zoff(sgn * d)])
        else:
            stats(7, [zoff(4)])

    scopies = []
    for k in range(1, NZ):
        cp = rcopy(STL, ST.at[k], st_s.at[k - 1], st_r.at[k - 1], {"seq": dev(y, zoff(k), c)})
        cp.start()
        scopies.append(cp)
    ST[0] = STL[...]
    for cp in scopies:
        cp.wait_recv()

    def add(k, total):
        return total + ST[(z + 2 * NZ - k) % NZ]

    total = lax.fori_loop(0, NZ, add, jnp.zeros((2 * NZ, BLK), F32))
    token = lax.broadcasted_iota(jnp.int32, (NZ, BLK), 0) * (2 * BLK) + (
        lax.broadcasted_iota(jnp.int32, (NZ, BLK), 1) + (y * NZ * 2 + c) * BLK
    )
    per_token = jnp.where(token < vlen[0], jnp.log(total[:NZ]) - total[NZ:], 0.0)
    mine = lax.broadcasted_iota(jnp.int32, (NZ, BLK), 0) == z
    tl_out[...] = jnp.sum(jnp.where(mine, per_token, 0.0), 0, keepdims=True)
    PART[pl.ds(2 * y + c, 1)] = per_token[None]
    pc = []
    for k, to in enumerate((partner, near, diag)):
        s = PART.at[2 * y + c]
        cp = rcopy(s, s, p_s.at[k], p_r.at[k], to)
        cp.start()
        pc.append(cp)
    for cp in pc:
        cp.wait_recv()
    loss = jnp.sum(PART[0] + PART[1] + (PART[2] + PART[3])) / vlen[0].astype(F32)
    loss_out[...] = jnp.full((1, BLK), loss, F32)

    for cp in pc + scopies:
        cp.wait_send()
    for si in range(6):
        drain(si)
    halo0.wait_send()
    halo1.wait_send()
    for cp in tcopies + [t_other]:
        cp.wait_send()
    for k, n in ((0, 4), (1, 3)):
        s = HALL.at[pl.ds(0, n)]
        rcopy(s, s, h_s.at[k], h_r.at[0, 0], fwd).wait_send()


def on_device(
    embedded, w_qkv, w_out, w_pos, bias_content, bias_position, norm_gain, norm_offset,
    table, targets, valid_length,
):
    vmem = pl.BlockSpec(memory_space=pltpu.VMEM)
    hbm = pl.BlockSpec(memory_space=pl.ANY)
    smem = pl.BlockSpec(memory_space=pltpu.SMEM)
    DMA = pltpu.SemaphoreType.DMA
    hidden, token_loss, loss = pl.pallas_call(
        kernel,
        out_shape=(
            jax.ShapeDtypeStruct((BLK, D), BF),
            jax.ShapeDtypeStruct((1, BLK), F32),
            jax.ShapeDtypeStruct((1, BLK), F32),
        ),
        in_specs=[hbm] * 5 + [vmem] * 4 + [hbm, vmem, smem],
        out_specs=(vmem, vmem, vmem),
        scratch_shapes=[
            pltpu.VMEM((LAYERS, 2, NZ, 2, SHARD, 3 * D), BF),
            pltpu.VMEM((LAYERS, 2, NZ, 2, SHARD, PO), BF),
            pltpu.VMEM((2, 2, WORDS, D), BF),
            pltpu.VMEM((2, BLK, D), BF),
            pltpu.VMEM((2, BLK, D), BF),
            pltpu.VMEM((BLK, D), BF),
            pltpu.VMEM((BLK, D), BF),
            pltpu.VMEM((2 * BLK, D), BF),
            pltpu.VMEM((2 * BLK, D), BF),
            pltpu.VMEM((BLK, D), BF),
            pltpu.VMEM((BLK, D), F32),
            pltpu.VMEM((NZ, BLK, D), BF),
            pltpu.VMEM((2 * NZ, BLK), F32),
            pltpu.VMEM((NZ, 2 * NZ, BLK), F32),
            pltpu.VMEM((4, NZ, BLK), F32),
            pltpu.VMEM((LAYERS, SHARD, D), BF),
            pltpu.VMEM((D, 2 * BLK), BF),
            DMA((7,)),
            DMA((6, 7)),
            DMA((6, 8)),
            DMA((6, 4)),
            DMA((6, 4)),
            DMA((6, 10)),
            DMA((2,)),
            DMA((2,)),
            DMA((4,)),
            DMA((4,)),
            DMA((2,)),
            DMA((7, 2)),
            DMA((NZ - 1,)),
            DMA((NZ - 1,)),
            DMA((3,)),
            DMA((3,)),
        ],
        compiler_params=pltpu.CompilerParams(
            collective_id=0, has_side_effects=True, vmem_limit_bytes=58 * 1024 * 1024
        ),
    )(
        embedded, w_qkv, w_out, jnp.swapaxes(w_pos, 1, 2), pos_table_t(2 * BLK, D), bias_content, bias_position, norm_gain, norm_offset,
        table, targets.reshape(32, BLK), valid_length,
    )
    return hidden, token_loss.reshape(BLK), loss[0, :1]


def solution(mesh):
    in_specs = (
        P(("batch", "seq"), None),
        P(None, "seq", None),
        P(None, "seq", None),
        P(None, None, "seq"),
        P(),
        P(),
        P(),
        P(),
        P("seq", None),
        P("batch"),
        P("batch"),
    )
    out_specs = (P(("batch", "seq"), None), P(("batch", "seq")), P("batch"))
    return jax.shard_map(
        on_device, mesh=mesh, in_specs=in_specs, out_specs=out_specs, check_vma=False
    )
```

```python
import functools

import jax
import jax.numpy as jnp
import numpy as np
from jax import lax
from jax.experimental import pallas as pl
from jax.experimental.pallas import tpu as pltpu
from jax.sharding import PartitionSpec as P

HEADS = 16
LAYERS = 2
D = 1024
BLK = 128
NZ = 8
SHARD = 32
WORDS = 384
PO = 256 + D
EPS = 1e-05
MESH = pl.DeviceIdType.MESH
BF = jnp.bfloat16
F32 = jnp.float32


ORDER = (
    ("o", 0), ("o", 1), ("o", 2), ("f", 0, 1), ("b", 0, 1), ("y", 0, 0), ("f", 1, 1),
    ("b", 1, 1), ("f", 2, 1), ("b", 2, 1), ("y", 2, 0), ("y", 0, 4), ("f", 0, 2), ("b", 0, 2),
    ("y", 0, 1), ("f", 1, 2), ("b", 1, 2), ("y", 2, 4), ("f", 2, 2), ("b", 2, 2), ("y", 2, 1),
    ("y", 0, 5), ("f", 0, 3), ("b", 0, 3), ("y", 0, 2), ("f", 1, 3), ("b", 1, 3), ("o", 3),
    ("y", 2, 5), ("f", 2, 3), ("b", 2, 3), ("y", 2, 2), ("f", 0, 4), ("d", 0, 0), ("y", 0, 6),
    ("y", 0, 3), ("f", 1, 4), ("d", 1, 0), ("o", 5), ("b", 3, 1), ("f", 3, 1), ("y", 2, 6),
    ("f", 2, 4), ("d", 2, 0), ("o", 4), ("y", 3, 0), ("d", 0, 2), ("f", 5, 1), ("b", 5, 1),
    ("y", 0, 7), ("d", 0, 1), ("y", 2, 3), ("b", 3, 2), ("d", 1, 1), ("f", 3, 2), ("o", 6),
    ("y", 3, 1), ("b", 4, 1), ("b", 5, 2), ("y", 3, 4), ("f", 4, 1), ("f", 5, 2), ("d", 2, 2),
    ("b", 3, 3), ("y", 2, 7), ("d", 2, 1), ("d", 0, 3), ("b", 6, 1), ("f", 3, 3), ("y", 3, 2),
    ("y", 3, 5), ("f", 6, 1), ("b", 4, 2), ("y", 6, 0), ("b", 5, 3), ("c", "q0"), ("f", 4, 2),
    ("c", "v0"), ("d", 2, 3), ("f", 3, 4), ("d", 3, 0), ("f", 5, 3), ("b", 6, 2), ("y", 3, 6),
    ("f", 6, 2), ("y", 3, 3), ("b", 4, 3), ("y", 6, 4), ("c", "a00"), ("f", 4, 3), ("y", 6, 1),
    ("c", "a01"), ("f", 5, 4), ("d", 5, 0), ("c", "a02"), ("f", 6, 3), ("b", 6, 3),
    ("c", "a03"), ("y", 3, 7), ("d", 3, 1), ("d", 3, 2), ("c", "p0"), ("y", 6, 2), ("f", 4, 4),
    ("d", 4, 0), ("c", "n0"), ("y", 6, 5), ("f", 6, 4), ("d", 6, 0), ("t", 0), ("y", 6, 3),
    ("d", 5, 1), ("y", 6, 6), ("d", 3, 3), ("d", 4, 1), ("d", 6, 2), ("y", 6, 7), ("d", 6, 1),
    ("c", "q1"), ("c", "k1"), ("c", "m1"), ("c", "a10"), ("d", 6, 3), ("c", "a11"),
    ("c", "a12"), ("c", "a13"), ("c", "p1"), ("c", "n1"),
)


def pos_table_t(row_count, model_width):
    distance = np.arange(row_count - 1, -1, -1).astype(np.float32)
    inverse = np.float32(1.0) / np.float32(10000.0) ** (
        np.arange(0, model_width, 2).astype(np.float32) / np.float32(model_width)
    )
    angles = distance[:, None] * inverse[None, :].astype(np.float32)
    table = np.concatenate([np.sin(angles), np.cos(angles)], axis=1)
    return jnp.asarray(table.T, F32).astype(BF)


def kernel(
    emb, wqkv, w_out, w_pos, ptab, bias_c, bias_p, gain, offset, table, targets, vlen,
    hid_out, tl_out, loss_out,
    W, POW, T, X0, X1, QC, QP, K, V, ATT, Y, HALL, STL, ST, PART, WP, PT,
    lsem, ring_r, y_r, x_r, d_r, w_s, halo_s, halo_r, t_s, t_r, h_s, h_r, st_s, st_r, p_s, p_r,
):
    i = lax.axis_index("seq")
    b = lax.axis_index("batch")
    c = i % 2
    z = (i // 2) % NZ
    y = i // (2 * NZ)
    sgn = 1 - 2 * c

    def dev(yy, zz, cc):
        return (yy * NZ + zz) * 2 + cc

    def zoff(k):
        return (z + 2 * NZ + k) % NZ

    fwd = {"seq": dev(y, zoff(sgn), c)}
    bwd = {"seq": dev(y, zoff(-sgn), c)}
    partner = {"seq": dev(y, z, 1 - c)}
    diag = {"seq": dev(1 - y, z, 1 - c)}
    near = {"seq": dev(1 - y, z, c)}
    far = {"seq": dev(1 - y, z, c), "batch": (b // 2) * 2 + 1 - b % 2}
    nxt = {"seq": (i + 1) % 32}
    prv = {"seq": (i + 31) % 32}
    x = b // 2
    xp = x % 2
    right = {"batch": ((x + 1) % 4) * 2 + b % 2}
    left = {"batch": ((x + 3) % 4) * 2 + b % 2}

    def rcopy(src, dst, ss, rs, to):
        return pltpu.make_async_remote_copy(
            src_ref=src, dst_ref=dst, send_sem=ss, recv_sem=rs, device_id=to, device_id_type=MESH
        )

    loc = [
        pltpu.make_async_copy(wqkv.at[0], W.at[0, y, z, c], lsem.at[0]),
        pltpu.make_async_copy(emb, X0.at[1], lsem.at[1]),
        pltpu.make_async_copy(w_pos, WP, lsem.at[2]),
        pltpu.make_async_copy(ptab, PT, lsem.at[3]),
        pltpu.make_async_copy(w_out, POW.at[:, y, z, c, :, pl.ds(256, D)], lsem.at[4]),
        pltpu.make_async_copy(wqkv.at[1], W.at[1, y, z, c], lsem.at[5]),
        pltpu.make_async_copy(table, T.at[y, c], lsem.at[6]),
    ]
    for cp in loc:
        cp.start()

    barrier = pltpu.get_barrier_semaphore()
    for peer in (fwd, bwd, partner, diag, near, far, nxt, prv, right, left):
        pl.semaphore_signal(barrier, inc=1, device_id=peer, device_id_type=MESH)
    pl.semaphore_wait(barrier, 10)

    def piece(si, yy, zz, kind):
        layer = si // 3 if si < 6 else 1
        if si == 5:
            return POW.at[1, yy, zz, c, :, pl.ds(0, 256)]
        if si in (2, 6):
            first, wide = (0, 896) if si == 2 else (256, 640)
            at, size = {"ring": (xp * 384, wide), "give": (xp * wide, 384), "take": ((1 - xp) * wide, 384)}[kind]
            return POW.at[layer, yy, zz, c, :, pl.ds(pl.multiple_of(first + at, 128), size)]
        if si % 3 == 1:
            return W.at[layer, yy, zz, c, :, pl.ds(D, D)]
        at = (1 - xp if kind == "take" else xp) * 2 * D
        return W.at[layer, yy, zz, c, :, pl.ds(pl.multiple_of(at, D), D)]

    def shares(si):
        return si in (0, 2, 3, 6)

    def place(k):
        return zoff(sgn * k) if k < 4 else zoff(-sgn * (k - 3))

    def ring_copy(si, zz, to, k):
        s = piece(si, y, zz, "ring")
        return rcopy(s, s, w_s.at[si, 0 if k < 4 else 1], ring_r.at[si, k], to)

    def y_copy(si, k):
        s = piece(si, y, place(k), "ring")
        slot = k if shares(si) else k // 4 * 4
        return rcopy(s, s, w_s.at[si, 2 + k // 4], y_r.at[si, slot], far if k >= 4 else near)

    def x_copy(si, yy, k, other):
        s = piece(si, yy, place(k), "give")
        return rcopy(s, s, w_s.at[si, 4 + k // 4], x_r.at[si, 2 * other + k // 4], left if k >= 4 else right)

    def d_copy(si, n):
        s = piece(si, y if n % 2 == 0 else 1 - y, pl.ds(0, NZ), "ring" if n < 2 else "take")
        return rcopy(s, s, w_s.at[si, 6 + n], d_r.at[si, n], partner)

    def several(si, kind, recv, n=4):
        s = piece(si, y, pl.ds(0, n), kind)
        return rcopy(s, s, w_s.at[si, 0], recv, partner)

    def own(si):
        ring_copy(si, z, fwd, 0).start()
        ring_copy(si, z, bwd, 4).start()
        y_copy(si, 0).start()

    def forward(si, d):
        zz = zoff(-sgn * d)
        ring_copy(si, zz, fwd, d - 1).wait_recv()
        if d < 4:
            ring_copy(si, zz, fwd, d).start()
        y_copy(si, 3 + d).start()
        if shares(si):
            x_copy(si, y, 3 + d, 0).start()

    def backward(si, d):
        zz = zoff(sgn * d)
        ring_copy(si, zz, bwd, 3 + d).wait_recv()
        if d < 3:
            ring_copy(si, zz, bwd, 4 + d).start()
        y_copy(si, d).start()
        if shares(si):
            x_copy(si, y, d, 0).start()

    def across(si, k):
        y_copy(si, k).wait_recv()
        x_copy(si, 1 - y, k, 1).start()

    def to_partner(si, n):
        if n == 1 and not shares(si):
            several(si, "ring", y_r.at[si, 0]).wait_recv()
            several(si, "ring", y_r.at[si, 4]).wait_recv()
        if n >= 2:
            several(si, "take", x_r.at[si, 2 * n - 4], n + 1).wait_recv()
            several(si, "take", x_r.at[si, 2 * n - 3]).wait_recv()
        d_copy(si, n).start()

    def finish(si):
        for n in range(4 if shares(si) else 2):
            d_copy(si, n).wait_recv()

    def drain(si):
        waits = [("ring", 0, 4), ("ring", 1, 3), ("ring", 2, 4), ("ring", 3, 4), ("ring", 6, 8), ("ring", 7, 8)]
        if shares(si):
            waits += [("give", 4, 7), ("give", 5, 8), ("take", 8, 8), ("take", 9, 8)]
        for kind, k, n in waits:
            s = piece(si, y, pl.ds(0, n), kind)
            rcopy(s, s, w_s.at[si, k], ring_r.at[si, 0], fwd).wait_send()

    low = lax.broadcasted_iota(jnp.int32, (BLK, BLK), 1) < 64
    rows = lax.broadcasted_iota(jnp.int32, (BLK, 2 * BLK), 0)
    cols = lax.broadcasted_iota(jnp.int32, (BLK, 2 * BLK), 1)
    first_key = BLK * (1 - jnp.minimum(i, 1))
    allowed = (cols <= rows + BLK) & (cols >= first_key)

    def lanes(t, size):
        return pl.ds(pl.multiple_of(t * size, size), size)

    def weights(layer, col):
        return W[layer, :, :, :, :, pl.ds(pl.multiple_of(col, 256), 256)].reshape(D, 256)

    def queries(layer, X):
        def body(t, carry):
            sl = lanes(t, 256)
            q = jnp.dot(X[1], weights(layer, t * 256), preferred_element_type=F32)
            QC[:, sl] = (q + bias_c[layer : layer + 1, sl]).astype(BF)
            QP[:, sl] = (q + bias_p[layer : layer + 1, sl]).astype(BF)
            return carry

        lax.fori_loop(0, 4, body, 0)

    def keys_values(layer, X, part):
        row0, count = {"all": (0, 2), "own": (1, 1), "memory": (0, 1)}[part]

        def body(t, carry):
            x = X[row0 : row0 + count].reshape(count * BLK, D)
            r = pl.ds(row0 * BLK, count * BLK)
            sl = lanes(t, 256)
            K[r, sl] = jnp.dot(x, weights(layer, D + t * 256), preferred_element_type=F32).astype(BF)
            V[r, sl] = jnp.dot(x, weights(layer, 2 * D + t * 256), preferred_element_type=F32).astype(BF)
            return carry

        lax.fori_loop(0, 4, body, 0)

    def both(x):
        zero = jnp.zeros_like(x)
        return jnp.concatenate([jnp.where(low, x, zero), jnp.where(low, zero, x)], 0)

    def attend(layer, start, stop):
        def body(p, carry):
            sl = lanes(p, BLK)
            q2 = both(QC[:, sl].astype(F32)).astype(BF)
            r2 = both(QP[:, sl].astype(F32)).astype(BF)
            content = lax.dot_general(
                q2, K[:, sl], (((1,), (1,)), ((), ())), preferred_element_type=F32
            )
            pos = POW[layer, p // 4, pl.ds((p % 4) * 2, 2), :, :, 0:256].reshape(BLK, 2 * BLK)
            position = jnp.dot(r2, pos, preferred_element_type=F32)
            outs = []
            for k in range(2):
                half = slice(k * BLK, (k + 1) * BLK)
                shifted = pltpu.roll(position[half], BLK + 1, 1, stride=1, stride_axis=0)
                scores = (content[half] + shifted) * 0.125
                e = jnp.where(allowed, jnp.exp(scores), 0.0)
                outs.append((e / jnp.sum(e, -1, keepdims=True)).astype(BF))
            o = jnp.dot(jnp.concatenate(outs, 0), V[:, sl], preferred_element_type=F32)
            ATT[:, sl] = jnp.where(low, o[:BLK], o[BLK:]).astype(BF)
            return carry

        lax.fori_loop(start, stop, body, 0)

    def project(layer, X):
        def body(t, carry):
            sl = lanes(t, 256)
            w = POW[layer, :, :, :, :, pl.ds(pl.multiple_of(256 + t * 256, 256), 256)].reshape(D, 256)
            Y[:, sl] = jnp.dot(ATT[...], w, preferred_element_type=F32) + X[1, :, sl].astype(F32)
            return carry

        lax.fori_loop(0, 4, body, 0)

    def norm(layer, dst, last):
        def body(t, carry):
            r = pl.ds(pl.multiple_of(t * 32, 32), 32)
            v = Y[r, :]
            v = v - jnp.mean(v, -1, keepdims=True)
            spread = jnp.mean(v * v, -1, keepdims=True)
            h = v * lax.rsqrt(spread + EPS) * gain[layer : layer + 1, :] + offset[layer : layer + 1, :]
            dst[r, :] = h.astype(BF)
            if last:
                pos = lax.broadcasted_iota(jnp.int32, (32, D), 0) + (i * BLK + t * 32)
                hid_out[r, :] = jnp.where(pos < vlen[0], h, 0.0).astype(BF)
            return carry

        lax.fori_loop(0, 4, body, 0)

    halves = (pl.ds(0, WORDS // 2), pl.ds(WORDS // 2, WORDS // 2))
    tcopies = [
        rcopy(T.at[y, c, h], T.at[y, c, h], t_s.at[k], t_r.at[k], to)
        for k, (h, to) in enumerate(zip(halves, (near, far)))
    ] + [rcopy(T.at[y, c], T.at[y, c], t_s.at[2], t_r.at[2], partner)]
    t_other = rcopy(T.at[1 - y, c], T.at[1 - y, c], t_s.at[3], t_r.at[3], partner)
    halo0 = rcopy(X0.at[1], X0.at[0], halo_s.at[0], halo_r.at[0], nxt)
    halo1 = rcopy(X1.at[1], X1.at[0], halo_s.at[1], halo_r.at[1], nxt)

    def table_step(n):
        if n == 0:
            for cp in tcopies:
                cp.start()
        else:
            tcopies[0].wait_recv()
            tcopies[1].wait_recv()
            t_other.start()

    def compute(name):
        kind, layer = name[0], int(name[1])
        X = (X0, X1)[layer]
        if name == "q0":
            finish(0)
            finish(1)
            queries(0, X0)
        elif name == "v0":
            halo0.wait_recv()
            keys_values(0, X0, "all")
        elif name == "q1":
            finish(3)
            finish(4)
            queries(1, X1)
        elif name == "k1":
            keys_values(1, X1, "own")
        elif name == "m1":
            halo1.wait_recv()
            keys_values(1, X1, "memory")
        elif kind == "a":
            k = int(name[2])
            if k == 0:
                finish(2 + 3 * layer)
            attend(layer, 2 * k, 2 * k + 2)
        elif kind == "p":
            if layer == 1:
                finish(6)
            project(layer, X)
        elif name == "n0":
            norm(0, X1.at[1], False)
            halo1.start()
        else:
            norm(1, HALL.at[0], True)

    def start_rest():
        loc[1].wait()
        loc[2].wait()
        loc[3].wait()
        for layer in range(LAYERS):
            share = lax.dot_general(
                WP[layer], PT[...], (((1,), (0,)), ((), ())), preferred_element_type=F32
            )
            POW[layer, y, z, c, :, 0:256] = share.astype(BF)
        for cp in loc[4:]:
            cp.wait()

    handlers = {"o": own, "f": forward, "b": backward, "y": across, "d": to_partner, "t": table_step}
    loc[0].wait()
    for n, (kind, *at) in enumerate(ORDER):
        if kind == "c":
            compute(at[0])
        else:
            handlers[kind](*at)
        if n == 1:
            start_rest()
        if ORDER[n] == ("f", 1, 4):
            halo0.start()

    hv = (pl.ds(0, BLK // 2), pl.ds(BLK // 2, BLK // 2))

    def hcopy(d, backward, half):
        src = 0 if d == 0 else (2 * d if backward else 2 * d - 1)
        dst = 2 * d + 2 if backward else 2 * d + 1
        k = (4 if backward else 0) + d
        return rcopy(
            HALL.at[src, hv[half]], HALL.at[dst, hv[half]],
            h_s.at[1 if backward else 0], h_r.at[k, half], bwd if backward else fwd,
        )

    for half in (0, 1):
        hcopy(0, False, half).start()
        hcopy(0, True, half).start()

    table_step(1)

    def stats(slot, blocks):
        n = len(blocks)
        hb = HALL[slot : slot + n].reshape(n * BLK, D)
        tg = [targets[pl.ds(dev(y, zz, c), 1), :] for zz in blocks]
        tg = tg[0] if n == 1 else jnp.concatenate(tg, 1)
        word = lax.broadcasted_iota(jnp.int32, (WORDS, n * BLK), 0)

        def body(k, carry):
            sums, picks = carry
            first = dev(k // 2, z, k % 2) * WORDS
            logits = lax.dot_general(
                T[k // 2, k % 2], hb, (((1,), (1,)), ((), ())), preferred_element_type=F32
            )
            sums = sums + jnp.sum(jnp.exp(logits), 0, keepdims=True)
            picks = picks + jnp.sum(jnp.where(word == tg - first, logits, 0.0), 0, keepdims=True)
            return sums, picks

        zero = jnp.zeros((1, n * BLK), F32)
        sums, picks = lax.fori_loop(0, 4, body, (zero, zero))
        for k, zz in enumerate(blocks):
            STL[pl.ds(zz, 1), :] = sums[:, k * BLK : (k + 1) * BLK]
            STL[pl.ds(NZ + zz, 1), :] = picks[:, k * BLK : (k + 1) * BLK]

    for d in (1, 2, 3, 4):
        for half in (0, 1):
            hcopy(d - 1, False, half).wait_recv()
            if d < 4:
                hcopy(d, False, half).start()
                hcopy(d - 1, True, half).wait_recv()
                if d < 3:
                    hcopy(d, True, half).start()
        if d == 1:
            tcopies[2].wait_recv()
            t_other.wait_recv()
            stats(0, [z])
        if d < 4:
            stats(2 * d - 1, [zoff(-sgn * d), zoff(sgn * d)])
        else:
            stats(7, [zoff(4)])

    scopies = []
    for k in range(1, NZ):
        cp = rcopy(STL, ST.at[k], st_s.at[k - 1], st_r.at[k - 1], {"seq": dev(y, zoff(k), c)})
        cp.start()
        scopies.append(cp)
    ST[0] = STL[...]
    for cp in scopies:
        cp.wait_recv()

    def add(k, total):
        return total + ST[(z + 2 * NZ - k) % NZ]

    total = lax.fori_loop(0, NZ, add, jnp.zeros((2 * NZ, BLK), F32))
    token = lax.broadcasted_iota(jnp.int32, (NZ, BLK), 0) * (2 * BLK) + (
        lax.broadcasted_iota(jnp.int32, (NZ, BLK), 1) + (y * NZ * 2 + c) * BLK
    )
    per_token = jnp.where(token < vlen[0], jnp.log(total[:NZ]) - total[NZ:], 0.0)
    mine = lax.broadcasted_iota(jnp.int32, (NZ, BLK), 0) == z
    tl_out[...] = jnp.sum(jnp.where(mine, per_token, 0.0), 0, keepdims=True)
    PART[pl.ds(2 * y + c, 1)] = per_token[None]
    pc = []
    for k, to in enumerate((partner, near, diag)):
        s = PART.at[2 * y + c]
        cp = rcopy(s, s, p_s.at[k], p_r.at[k], to)
        cp.start()
        pc.append(cp)
    for cp in pc:
        cp.wait_recv()
    loss = jnp.sum(PART[0] + PART[1] + (PART[2] + PART[3])) / vlen[0].astype(F32)
    loss_out[...] = jnp.full((1, BLK), loss, F32)

    for cp in pc + scopies:
        cp.wait_send()
    for si in range(7):
        drain(si)
    halo0.wait_send()
    halo1.wait_send()
    for cp in tcopies + [t_other]:
        cp.wait_send()
    for k, n in ((0, 4), (1, 3)):
        s = HALL.at[pl.ds(0, n)]
        rcopy(s, s, h_s.at[k], h_r.at[0, 0], fwd).wait_send()


def on_device(
    embedded, w_qkv, w_out, w_pos, bias_content, bias_position, norm_gain, norm_offset,
    table, targets, valid_length,
):
    vmem = pl.BlockSpec(memory_space=pltpu.VMEM)
    hbm = pl.BlockSpec(memory_space=pl.ANY)
    smem = pl.BlockSpec(memory_space=pltpu.SMEM)
    DMA = pltpu.SemaphoreType.DMA
    hidden, token_loss, loss = pl.pallas_call(
        kernel,
        out_shape=(
            jax.ShapeDtypeStruct((BLK, D), BF),
            jax.ShapeDtypeStruct((1, BLK), F32),
            jax.ShapeDtypeStruct((1, BLK), F32),
        ),
        in_specs=[hbm] * 5 + [vmem] * 4 + [hbm, vmem, smem],
        out_specs=(vmem, vmem, vmem),
        scratch_shapes=[
            pltpu.VMEM((LAYERS, 2, NZ, 2, SHARD, 3 * D), BF),
            pltpu.VMEM((LAYERS, 2, NZ, 2, SHARD, PO), BF),
            pltpu.VMEM((2, 2, WORDS, D), BF),
            pltpu.VMEM((2, BLK, D), BF),
            pltpu.VMEM((2, BLK, D), BF),
            pltpu.VMEM((BLK, D), BF),
            pltpu.VMEM((BLK, D), BF),
            pltpu.VMEM((2 * BLK, D), BF),
            pltpu.VMEM((2 * BLK, D), BF),
            pltpu.VMEM((BLK, D), BF),
            pltpu.VMEM((BLK, D), F32),
            pltpu.VMEM((NZ, BLK, D), BF),
            pltpu.VMEM((2 * NZ, BLK), F32),
            pltpu.VMEM((NZ, 2 * NZ, BLK), F32),
            pltpu.VMEM((4, NZ, BLK), F32),
            pltpu.VMEM((LAYERS, SHARD, D), BF),
            pltpu.VMEM((D, 2 * BLK), BF),
            DMA((7,)),
            DMA((7, 7)),
            DMA((7, 8)),
            DMA((7, 4)),
            DMA((7, 4)),
            DMA((7, 10)),
            DMA((2,)),
            DMA((2,)),
            DMA((4,)),
            DMA((4,)),
            DMA((2,)),
            DMA((7, 2)),
            DMA((NZ - 1,)),
            DMA((NZ - 1,)),
            DMA((3,)),
            DMA((3,)),
        ],
        compiler_params=pltpu.CompilerParams(
            collective_id=0, has_side_effects=True, vmem_limit_bytes=58 * 1024 * 1024
        ),
    )(
        embedded, w_qkv, w_out, jnp.swapaxes(w_pos, 1, 2), pos_table_t(2 * BLK, D), bias_content, bias_position, norm_gain, norm_offset,
        table, targets.reshape(32, BLK), valid_length,
    )
    return hidden, token_loss.reshape(BLK), loss[0, :1]


def solution(mesh):
    in_specs = (
        P(("batch", "seq"), None),
        P(None, "seq", None),
        P(None, "seq", None),
        P(None, None, "seq"),
        P(),
        P(),
        P(),
        P(),
        P("seq", None),
        P("batch"),
        P("batch"),
    )
    out_specs = (P(("batch", "seq"), None), P(("batch", "seq")), P("batch"))
    return jax.shard_map(
        on_device, mesh=mesh, in_specs=in_specs, out_specs=out_specs, check_vma=False
    )
```

```python
import functools

import jax
import jax.numpy as jnp
import numpy as np
from jax import lax
from jax.experimental import pallas as pl
from jax.experimental.pallas import tpu as pltpu
from jax.sharding import PartitionSpec as P

HEADS = 16
LAYERS = 2
D = 1024
BLK = 128
NZ = 8
SHARD = 32
WORDS = 384
PO = 256 + D
EPS = 1e-05
MESH = pl.DeviceIdType.MESH
BF = jnp.bfloat16
F32 = jnp.float32


ORDER = (
    ("o", 0), ("o", 1), ("o", 2), ("f", 0, 1), ("b", 0, 1), ("y", 0, 0), ("f", 1, 1),
    ("b", 1, 1), ("f", 2, 1), ("b", 2, 1), ("y", 2, 0), ("y", 0, 4), ("f", 0, 2), ("b", 0, 2),
    ("y", 0, 1), ("f", 1, 2), ("b", 1, 2), ("y", 2, 4), ("f", 2, 2), ("b", 2, 2), ("y", 2, 1),
    ("y", 0, 5), ("f", 0, 3), ("b", 0, 3), ("y", 0, 2), ("f", 1, 3), ("b", 1, 3), ("o", 3),
    ("y", 2, 5), ("f", 2, 3), ("b", 2, 3), ("y", 2, 2), ("f", 0, 4), ("d", 0, 0), ("y", 0, 6),
    ("y", 0, 3), ("f", 1, 4), ("d", 1, 0), ("o", 5), ("b", 3, 1), ("f", 3, 1), ("y", 2, 6),
    ("f", 2, 4), ("d", 2, 0), ("o", 4), ("y", 3, 0), ("d", 0, 2), ("f", 5, 1), ("b", 5, 1),
    ("y", 0, 7), ("d", 0, 1), ("y", 2, 3), ("b", 3, 2), ("d", 1, 1), ("f", 3, 2), ("o", 6),
    ("y", 3, 1), ("b", 4, 1), ("b", 5, 2), ("y", 3, 4), ("f", 4, 1), ("f", 5, 2), ("d", 2, 2),
    ("b", 3, 3), ("y", 2, 7), ("d", 2, 1), ("d", 0, 3), ("b", 6, 1), ("f", 3, 3), ("y", 3, 2),
    ("y", 3, 5), ("f", 6, 1), ("b", 4, 2), ("y", 6, 0), ("b", 5, 3), ("c", "q0"), ("f", 4, 2),
    ("c", "v0"), ("d", 2, 3), ("f", 3, 4), ("d", 3, 0), ("f", 5, 3), ("b", 6, 2), ("y", 3, 6),
    ("f", 6, 2), ("y", 3, 3), ("b", 4, 3), ("y", 6, 4), ("c", "a00"), ("f", 4, 3), ("y", 6, 1),
    ("c", "a01"), ("f", 5, 4), ("d", 5, 0), ("c", "a02"), ("f", 6, 3), ("b", 6, 3),
    ("c", "a03"), ("y", 3, 7), ("d", 3, 1), ("d", 3, 2), ("c", "p0"), ("y", 6, 2), ("f", 4, 4),
    ("d", 4, 0), ("c", "n0"), ("y", 6, 5), ("f", 6, 4), ("d", 6, 0), ("t", 0), ("y", 6, 3),
    ("d", 5, 1), ("y", 6, 6), ("d", 3, 3), ("d", 4, 1), ("d", 6, 2), ("y", 6, 7), ("d", 6, 1),
    ("c", "q1"), ("c", "k1"), ("c", "m1"), ("c", "a10"), ("d", 6, 3), ("c", "a11"),
    ("c", "a12"), ("c", "a13"), ("c", "p1"), ("c", "n1"),
)


def pos_table_t(row_count, model_width):
    distance = np.arange(row_count - 1, -1, -1).astype(np.float32)
    inverse = np.float32(1.0) / np.float32(10000.0) ** (
        np.arange(0, model_width, 2).astype(np.float32) / np.float32(model_width)
    )
    angles = distance[:, None] * inverse[None, :].astype(np.float32)
    table = np.concatenate([np.sin(angles), np.cos(angles)], axis=1)
    return jnp.asarray(table.T, F32).astype(BF)


def kernel(
    emb, wqkv, w_out, w_pos, ptab, bias_c, bias_p, gain, offset, table, targets, vlen,
    hid_out, tl_out, loss_out,
    W, POW, T, X0, X1, QC, QP, K, V, ATT, Y, HALL, STL, ST, PART, WP, PT,
    lsem, ring_r, y_r, x_r, d_r, w_s, halo_s, halo_r, t_s, t_r, h_s, h_r, st_s, st_r, p_s, p_r,
):
    i = lax.axis_index("seq")
    b = lax.axis_index("batch")
    c = i % 2
    z = (i // 2) % NZ
    y = i // (2 * NZ)
    sgn = 1 - 2 * c

    def dev(yy, zz, cc):
        return (yy * NZ + zz) * 2 + cc

    def zoff(k):
        return (z + 2 * NZ + k) % NZ

    fwd = {"seq": dev(y, zoff(sgn), c)}
    bwd = {"seq": dev(y, zoff(-sgn), c)}
    partner = {"seq": dev(y, z, 1 - c)}
    diag = {"seq": dev(1 - y, z, 1 - c)}
    near = {"seq": dev(1 - y, z, c)}
    far = {"seq": dev(1 - y, z, c), "batch": (b // 2) * 2 + 1 - b % 2}
    nxt = {"seq": (i + 1) % 32}
    prv = {"seq": (i + 31) % 32}
    x = b // 2
    xp = x % 2
    right = {"batch": ((x + 1) % 4) * 2 + b % 2}
    left = {"batch": ((x + 3) % 4) * 2 + b % 2}

    def rcopy(src, dst, ss, rs, to):
        return pltpu.make_async_remote_copy(
            src_ref=src, dst_ref=dst, send_sem=ss, recv_sem=rs, device_id=to, device_id_type=MESH
        )

    loc = [
        pltpu.make_async_copy(wqkv.at[0], W.at[0, y, z, c], lsem.at[0]),
        pltpu.make_async_copy(emb, X0.at[1], lsem.at[1]),
        pltpu.make_async_copy(w_pos, WP, lsem.at[2]),
        pltpu.make_async_copy(ptab, PT, lsem.at[3]),
        pltpu.make_async_copy(w_out, POW.at[:, y, z, c, :, pl.ds(256, D)], lsem.at[4]),
        pltpu.make_async_copy(wqkv.at[1], W.at[1, y, z, c], lsem.at[5]),
        pltpu.make_async_copy(table, T.at[y, c], lsem.at[6]),
    ]
    for cp in loc:
        cp.start()

    barrier = pltpu.get_barrier_semaphore()
    for peer in (fwd, bwd, partner, diag, near, far, nxt, prv, right, left):
        pl.semaphore_signal(barrier, inc=1, device_id=peer, device_id_type=MESH)
    pl.semaphore_wait(barrier, 10)

    def piece(si, yy, zz, kind):
        layer = si // 3 if si < 6 else 1
        if si == 5:
            return POW.at[1, yy, zz, c, :, pl.ds(0, 256)]
        if si in (2, 6):
            first, wide = (0, 896) if si == 2 else (256, 640)
            at, size = {"ring": (xp * 384, wide), "give": (xp * wide, 384), "take": ((1 - xp) * wide, 384)}[kind]
            return POW.at[layer, yy, zz, c, :, pl.ds(pl.multiple_of(first + at, 128), size)]
        if si % 3 == 1:
            return W.at[layer, yy, zz, c, :, pl.ds(D, D)]
        at = (1 - xp if kind == "take" else xp) * 2 * D
        return W.at[layer, yy, zz, c, :, pl.ds(pl.multiple_of(at, D), D)]

    def shares(si):
        return si in (0, 2, 3, 6)

    def place(k):
        return zoff(sgn * k) if k < 4 else zoff(-sgn * (k - 3))

    def ring_copy(si, zz, to, k):
        s = piece(si, y, zz, "ring")
        return rcopy(s, s, w_s.at[si, 0 if k < 4 else 1], ring_r.at[si, k], to)

    def y_copy(si, k):
        s = piece(si, y, place(k), "ring")
        slot = k if shares(si) else k // 4 * 4
        return rcopy(s, s, w_s.at[si, 2 + k // 4], y_r.at[si, slot], far if k >= 4 else near)

    def x_copy(si, yy, k, other):
        s = piece(si, yy, place(k), "give")
        return rcopy(s, s, w_s.at[si, 4 + k // 4], x_r.at[si, 2 * other + k // 4], left if k >= 4 else right)

    def d_copy(si, n):
        s = piece(si, y if n % 2 == 0 else 1 - y, pl.ds(0, NZ), "ring" if n < 2 else "take")
        return rcopy(s, s, w_s.at[si, 6 + n], d_r.at[si, n], partner)

    def several(si, kind, recv, n=4):
        s = piece(si, y, pl.ds(0, n), kind)
        return rcopy(s, s, w_s.at[si, 0], recv, partner)

    def own(si):
        ring_copy(si, z, fwd, 0).start()
        ring_copy(si, z, bwd, 4).start()
        y_copy(si, 0).start()

    def forward(si, d):
        zz = zoff(-sgn * d)
        ring_copy(si, zz, fwd, d - 1).wait_recv()
        if d < 4:
            ring_copy(si, zz, fwd, d).start()
        y_copy(si, 3 + d).start()
        if shares(si):
            x_copy(si, y, 3 + d, 0).start()

    def backward(si, d):
        zz = zoff(sgn * d)
        ring_copy(si, zz, bwd, 3 + d).wait_recv()
        if d < 3:
            ring_copy(si, zz, bwd, 4 + d).start()
        y_copy(si, d).start()
        if shares(si):
            x_copy(si, y, d, 0).start()

    def across(si, k):
        y_copy(si, k).wait_recv()
        x_copy(si, 1 - y, k, 1).start()

    def to_partner(si, n):
        if n == 1 and not shares(si):
            several(si, "ring", y_r.at[si, 0]).wait_recv()
            several(si, "ring", y_r.at[si, 4]).wait_recv()
        if n >= 2:
            several(si, "take", x_r.at[si, 2 * n - 4], n + 1).wait_recv()
            several(si, "take", x_r.at[si, 2 * n - 3]).wait_recv()
        d_copy(si, n).start()

    def finish(si):
        for n in range(4 if shares(si) else 2):
            d_copy(si, n).wait_recv()

    def drain(si):
        waits = [("ring", 0, 4), ("ring", 1, 3), ("ring", 2, 4), ("ring", 3, 4), ("ring", 6, 8), ("ring", 7, 8)]
        if shares(si):
            waits += [("give", 4, 7), ("give", 5, 8), ("take", 8, 8), ("take", 9, 8)]
        for kind, k, n in waits:
            s = piece(si, y, pl.ds(0, n), kind)
            rcopy(s, s, w_s.at[si, k], ring_r.at[si, 0], fwd).wait_send()

    low = lax.broadcasted_iota(jnp.int32, (BLK, BLK), 1) < 64
    rows = lax.broadcasted_iota(jnp.int32, (BLK, 2 * BLK), 0)
    cols = lax.broadcasted_iota(jnp.int32, (BLK, 2 * BLK), 1)
    first_key = BLK * (1 - jnp.minimum(i, 1))
    allowed = (cols <= rows + BLK) & (cols >= first_key)

    def lanes(t, size):
        return pl.ds(pl.multiple_of(t * size, size), size)

    def weights(layer, col):
        return W[layer, :, :, :, :, pl.ds(pl.multiple_of(col, 256), 256)].reshape(D, 256)

    def queries(layer, X):
        def body(t, carry):
            sl = lanes(t, 256)
            q = jnp.dot(X[1], weights(layer, t * 256), preferred_element_type=F32)
            QC[:, sl] = (q + bias_c[layer : layer + 1, sl]).astype(BF)
            QP[:, sl] = (q + bias_p[layer : layer + 1, sl]).astype(BF)
            return carry

        lax.fori_loop(0, 4, body, 0)

    def keys_values(layer, X, part):
        row0, count = {"all": (0, 2), "own": (1, 1), "memory": (0, 1)}[part]

        def body(t, carry):
            x = X[row0 : row0 + count].reshape(count * BLK, D)
            r = pl.ds(row0 * BLK, count * BLK)
            sl = lanes(t, 256)
            K[r, sl] = jnp.dot(x, weights(layer, D + t * 256), preferred_element_type=F32).astype(BF)
            V[r, sl] = jnp.dot(x, weights(layer, 2 * D + t * 256), preferred_element_type=F32).astype(BF)
            return carry

        lax.fori_loop(0, 4, body, 0)

    def both(x):
        zero = jnp.zeros_like(x)
        return jnp.concatenate([jnp.where(low, x, zero), jnp.where(low, zero, x)], 0)

    def attend(layer, start, stop):
        def body(p, carry):
            sl = lanes(p, BLK)
            q2 = both(QC[:, sl].astype(F32)).astype(BF)
            r2 = both(QP[:, sl].astype(F32)).astype(BF)
            content = lax.dot_general(
                q2, K[:, sl], (((1,), (1,)), ((), ())), preferred_element_type=F32
            )
            pos = POW[layer, p // 4, pl.ds((p % 4) * 2, 2), :, :, 0:256].reshape(BLK, 2 * BLK)
            position = jnp.dot(r2, pos, preferred_element_type=F32)
            outs = []
            for k in range(2):
                half = slice(k * BLK, (k + 1) * BLK)
                shifted = pltpu.roll(position[half], BLK + 1, 1, stride=1, stride_axis=0)
                scores = (content[half] + shifted) * 0.125
                e = jnp.where(allowed, jnp.exp(scores), 0.0)
                outs.append((e / jnp.sum(e, -1, keepdims=True)).astype(BF))
            o = jnp.dot(jnp.concatenate(outs, 0), V[:, sl], preferred_element_type=F32)
            ATT[:, sl] = jnp.where(low, o[:BLK], o[BLK:]).astype(BF)
            return carry

        lax.fori_loop(start, stop, body, 0)

    def project(layer, X):
        def body(t, carry):
            sl = lanes(t, 256)
            w = POW[layer, :, :, :, :, pl.ds(pl.multiple_of(256 + t * 256, 256), 256)].reshape(D, 256)
            Y[:, sl] = jnp.dot(ATT[...], w, preferred_element_type=F32) + X[1, :, sl].astype(F32)
            return carry

        lax.fori_loop(0, 4, body, 0)

    hv = [pl.ds(k * BLK // 4, BLK // 4) for k in range(4)]

    def hcopy(d, backward, half):
        src = 0 if d == 0 else (2 * d if backward else 2 * d - 1)
        dst = 2 * d + 2 if backward else 2 * d + 1
        k = (4 if backward else 0) + d
        return rcopy(
            HALL.at[src, hv[half]], HALL.at[dst, hv[half]],
            h_s.at[1 if backward else 0], h_r.at[k, half], bwd if backward else fwd,
        )

    def norm(layer, dst, last):
        def body(t, carry):
            r = pl.ds(pl.multiple_of(t * 32, 32), 32)
            v = Y[r, :]
            v = v - jnp.mean(v, -1, keepdims=True)
            spread = jnp.mean(v * v, -1, keepdims=True)
            h = v * lax.rsqrt(spread + EPS) * gain[layer : layer + 1, :] + offset[layer : layer + 1, :]
            dst[r, :] = h.astype(BF)
            if last:
                pos = lax.broadcasted_iota(jnp.int32, (32, D), 0) + (i * BLK + t * 32)
                hid_out[r, :] = jnp.where(pos < vlen[0], h, 0.0).astype(BF)
            return carry

        if not last:
            lax.fori_loop(0, 4, body, 0)
            return
        for t in range(5):
            if t < 4:
                body(t, 0)
            if t > 0:
                hcopy(0, False, t - 1).start()
                hcopy(0, True, t - 1).start()

    halves = (pl.ds(0, WORDS // 2), pl.ds(WORDS // 2, WORDS // 2))
    tcopies = [
        rcopy(T.at[y, c, h], T.at[y, c, h], t_s.at[k], t_r.at[k], to)
        for k, (h, to) in enumerate(zip(halves, (near, far)))
    ] + [rcopy(T.at[y, c], T.at[y, c], t_s.at[2], t_r.at[2], partner)]
    t_other = rcopy(T.at[1 - y, c], T.at[1 - y, c], t_s.at[3], t_r.at[3], partner)
    halo0 = rcopy(X0.at[1], X0.at[0], halo_s.at[0], halo_r.at[0], nxt)
    halo1 = rcopy(X1.at[1], X1.at[0], halo_s.at[1], halo_r.at[1], nxt)

    def table_step(n):
        if n == 0:
            for cp in tcopies:
                cp.start()
        else:
            tcopies[0].wait_recv()
            tcopies[1].wait_recv()
            t_other.start()

    def compute(name):
        kind, layer = name[0], int(name[1])
        X = (X0, X1)[layer]
        if name == "q0":
            finish(0)
            finish(1)
            queries(0, X0)
        elif name == "v0":
            halo0.wait_recv()
            keys_values(0, X0, "all")
        elif name == "q1":
            finish(3)
            finish(4)
            queries(1, X1)
        elif name == "k1":
            keys_values(1, X1, "own")
        elif name == "m1":
            halo1.wait_recv()
            keys_values(1, X1, "memory")
        elif kind == "a":
            k = int(name[2])
            if k == 0:
                finish(2 + 3 * layer)
            attend(layer, 2 * k, 2 * k + 2)
        elif kind == "p":
            if layer == 1:
                finish(6)
            project(layer, X)
        elif name == "n0":
            norm(0, X1.at[1], False)
            halo1.start()
        else:
            norm(1, HALL.at[0], True)

    def start_rest():
        loc[1].wait()
        loc[2].wait()
        loc[3].wait()
        for layer in range(LAYERS):
            share = lax.dot_general(
                WP[layer], PT[...], (((1,), (0,)), ((), ())), preferred_element_type=F32
            )
            POW[layer, y, z, c, :, 0:256] = share.astype(BF)
        for cp in loc[4:]:
            cp.wait()

    handlers = {"o": own, "f": forward, "b": backward, "y": across, "d": to_partner, "t": table_step}
    loc[0].wait()
    for n, (kind, *at) in enumerate(ORDER):
        if kind == "c":
            compute(at[0])
        else:
            handlers[kind](*at)
        if n == 1:
            start_rest()
        if ORDER[n] == ("f", 1, 4):
            halo0.start()

    table_step(1)

    def stats(slot, blocks):
        n = len(blocks)
        hb = HALL[slot : slot + n].reshape(n * BLK, D)
        tg = [targets[pl.ds(dev(y, zz, c), 1), :] for zz in blocks]
        tg = tg[0] if n == 1 else jnp.concatenate(tg, 1)
        word = lax.broadcasted_iota(jnp.int32, (WORDS, n * BLK), 0)

        def body(k, carry):
            sums, picks = carry
            first = dev(k // 2, z, k % 2) * WORDS
            logits = lax.dot_general(
                T[k // 2, k % 2], hb, (((1,), (1,)), ((), ())), preferred_element_type=F32
            )
            sums = sums + jnp.sum(jnp.exp(logits), 0, keepdims=True)
            picks = picks + jnp.sum(jnp.where(word == tg - first, logits, 0.0), 0, keepdims=True)
            return sums, picks

        zero = jnp.zeros((1, n * BLK), F32)
        sums, picks = lax.fori_loop(0, 4, body, (zero, zero))
        for k, zz in enumerate(blocks):
            STL[pl.ds(zz, 1), :] = sums[:, k * BLK : (k + 1) * BLK]
            STL[pl.ds(NZ + zz, 1), :] = picks[:, k * BLK : (k + 1) * BLK]

    for d in (1, 2, 3, 4):
        for half in range(4):
            hcopy(d - 1, False, half).wait_recv()
            if d < 4:
                hcopy(d, False, half).start()
                hcopy(d - 1, True, half).wait_recv()
                if d < 3:
                    hcopy(d, True, half).start()
        if d == 1:
            tcopies[2].wait_recv()
            t_other.wait_recv()
            stats(0, [z])
        if d < 4:
            stats(2 * d - 1, [zoff(-sgn * d), zoff(sgn * d)])
        else:
            stats(7, [zoff(4)])

    scopies = []
    for k in range(1, NZ):
        cp = rcopy(STL, ST.at[k], st_s.at[k - 1], st_r.at[k - 1], {"seq": dev(y, zoff(k), c)})
        cp.start()
        scopies.append(cp)
    ST[0] = STL[...]
    for cp in scopies:
        cp.wait_recv()

    def add(k, total):
        return total + ST[(z + 2 * NZ - k) % NZ]

    total = lax.fori_loop(0, NZ, add, jnp.zeros((2 * NZ, BLK), F32))
    token = lax.broadcasted_iota(jnp.int32, (NZ, BLK), 0) * (2 * BLK) + (
        lax.broadcasted_iota(jnp.int32, (NZ, BLK), 1) + (y * NZ * 2 + c) * BLK
    )
    per_token = jnp.where(token < vlen[0], jnp.log(total[:NZ]) - total[NZ:], 0.0)
    mine = lax.broadcasted_iota(jnp.int32, (NZ, BLK), 0) == z
    tl_out[...] = jnp.sum(jnp.where(mine, per_token, 0.0), 0, keepdims=True)
    PART[pl.ds(2 * y + c, 1)] = per_token[None]
    pc = []
    for k, to in enumerate((partner, near, diag)):
        s = PART.at[2 * y + c]
        cp = rcopy(s, s, p_s.at[k], p_r.at[k], to)
        cp.start()
        pc.append(cp)
    for cp in pc:
        cp.wait_recv()
    loss = jnp.sum(PART[0] + PART[1] + (PART[2] + PART[3])) / vlen[0].astype(F32)
    loss_out[...] = jnp.full((1, BLK), loss, F32)

    for cp in pc + scopies:
        cp.wait_send()
    for si in range(7):
        drain(si)
    halo0.wait_send()
    halo1.wait_send()
    for cp in tcopies + [t_other]:
        cp.wait_send()
    for k, n in ((0, 4), (1, 3)):
        s = HALL.at[pl.ds(0, n)]
        rcopy(s, s, h_s.at[k], h_r.at[0, 0], fwd).wait_send()


def on_device(
    embedded, w_qkv, w_out, w_pos, bias_content, bias_position, norm_gain, norm_offset,
    table, targets, valid_length,
):
    vmem = pl.BlockSpec(memory_space=pltpu.VMEM)
    hbm = pl.BlockSpec(memory_space=pl.ANY)
    smem = pl.BlockSpec(memory_space=pltpu.SMEM)
    DMA = pltpu.SemaphoreType.DMA
    hidden, token_loss, loss = pl.pallas_call(
        kernel,
        out_shape=(
            jax.ShapeDtypeStruct((BLK, D), BF),
            jax.ShapeDtypeStruct((1, BLK), F32),
            jax.ShapeDtypeStruct((1, BLK), F32),
        ),
        in_specs=[hbm] * 5 + [vmem] * 4 + [hbm, vmem, smem],
        out_specs=(vmem, vmem, vmem),
        scratch_shapes=[
            pltpu.VMEM((LAYERS, 2, NZ, 2, SHARD, 3 * D), BF),
            pltpu.VMEM((LAYERS, 2, NZ, 2, SHARD, PO), BF),
            pltpu.VMEM((2, 2, WORDS, D), BF),
            pltpu.VMEM((2, BLK, D), BF),
            pltpu.VMEM((2, BLK, D), BF),
            pltpu.VMEM((BLK, D), BF),
            pltpu.VMEM((BLK, D), BF),
            pltpu.VMEM((2 * BLK, D), BF),
            pltpu.VMEM((2 * BLK, D), BF),
            pltpu.VMEM((BLK, D), BF),
            pltpu.VMEM((BLK, D), F32),
            pltpu.VMEM((NZ, BLK, D), BF),
            pltpu.VMEM((2 * NZ, BLK), F32),
            pltpu.VMEM((NZ, 2 * NZ, BLK), F32),
            pltpu.VMEM((4, NZ, BLK), F32),
            pltpu.VMEM((LAYERS, SHARD, D), BF),
            pltpu.VMEM((D, 2 * BLK), BF),
            DMA((7,)),
            DMA((7, 7)),
            DMA((7, 8)),
            DMA((7, 4)),
            DMA((7, 4)),
            DMA((7, 10)),
            DMA((2,)),
            DMA((2,)),
            DMA((4,)),
            DMA((4,)),
            DMA((2,)),
            DMA((7, 4)),
            DMA((NZ - 1,)),
            DMA((NZ - 1,)),
            DMA((3,)),
            DMA((3,)),
        ],
        compiler_params=pltpu.CompilerParams(
            collective_id=0, has_side_effects=True, vmem_limit_bytes=58 * 1024 * 1024
        ),
    )(
        embedded, w_qkv, w_out, jnp.swapaxes(w_pos, 1, 2), pos_table_t(2 * BLK, D), bias_content, bias_position, norm_gain, norm_offset,
        table, targets.reshape(32, BLK), valid_length,
    )
    return hidden, token_loss.reshape(BLK), loss[0, :1]


def solution(mesh):
    in_specs = (
        P(("batch", "seq"), None),
        P(None, "seq", None),
        P(None, "seq", None),
        P(None, None, "seq"),
        P(),
        P(),
        P(),
        P(),
        P("seq", None),
        P("batch"),
        P("batch"),
    )
    out_specs = (P(("batch", "seq"), None), P(("batch", "seq")), P("batch"))
    return jax.shard_map(
        on_device, mesh=mesh, in_specs=in_specs, out_specs=out_specs, check_vma=False
    )
```
